32 devices in a mesh: rows: 8 (over z, y), rep: 4 (over x, core).
Axes of the slice: x: 2, y: 2, z: 4, core: 2. Of those that a mesh axis runs over, the one named last changes fastest.
Arguments:
- field_in: bfloat16 [64, 384, 256], P('rows'), may hold values from -6 to 6
- left_factors: bfloat16 [1024, 384, 64], P(('rows', 'rep')), may hold values from -0.3125 to 0.3125
- right_factors: bfloat16 [1024, 384, 64], P(('rows', 'rep')), may hold values from -0.1875 to 0.1875
- block_ranks: int32 [1024], P(('rows', 'rep')), may hold values from 8 to 64
- row_cluster: int32 [1024], P(('rows', 'rep')), may hold values from 0 to 7
- col_owner: int32 [1024, 1], P(('rows', 'rep')), may hold values from 0 to 7; in each aligned block of 32 rows (0 to 31, 32 to 63, ...) at most 6 rows name the same one
- col_cluster: int32 [1024], P(('rows', 'rep')), may hold values from 0 to 7
- near_blocks: bfloat16 [64, 3, 384, 384], P('rows', None, 'rep'), may hold values from -0.1875 to 0.1875
Outputs:
- result_field: float32 [64, 384, 256], P('rows')
The draws below stay inside these ranges and needn't reach their ends.
Inputs may be any that keep to these rules, and one draw needn't show every extreme that they name: `col_owner`: among the 32 blocks of one device no owner is named more than once.
All inputs are finite; a program needn't handle non-finite values.
Results may differ from the reference program's by a relative error of at most 0.0029.
Values may be sent and summed in bfloat16 or wider, within the bound.
A program may use at most 128 MiB of HBM per device.

```python
import math
import jax
import jax.numpy as jnp
import numpy as np
from jax import lax

CL = 384
RANK = 64
NRHS = 256
BPD = 32
CPD = 8
NC = 64
NB = 1024
OWNERS = 8
MOST = 6
N_ROWS = 8
N_REP = 4


def place_ends(entries, key, least, largest):
    shape = entries.shape
    spot = [jax.random.randint(jax.random.fold_in(key, axis), (), 0, shape[axis]) for axis in range(len(shape))]
    entries = entries.at[tuple(spot)].set(least)
    longest = shape.index(max(shape))
    spot[longest] = (spot[longest] + 1) % shape[longest]
    return entries.at[tuple(spot)].set(largest)


def block_scale(rng, shape, shards, smallest, top_value):
    factor_of = 1.0
    for dim, parts in shards:
        heights = jax.random.uniform(jax.random.fold_in(jax.random.fold_in(rng, 6), dim), (parts,), jnp.float32, smallest / len(shards), top_value / len(shards))
        factor_of = factor_of * jnp.repeat(jnp.exp(heights), shape[dim] // parts).reshape((-1,) + (1,) * (len(shape) - 1 - dim))
    return factor_of


def routed_block(key, own, number, rows, count, top, limit, skew):
    sequence = jax.random.permutation(key, count)
    crowded, usual = shares(count, rows * top, limit, skew, True), shares(count, rows * top, limit, skew, False)
    places = jnp.arange(count)

    def named(tallies, rotation):
        used = int((tallies > 0).sum())
        fixed = max(1, used // 4)
        passed = fixed + (places - fixed + rotation * (used - fixed)) % max(1, count - fixed)
        return jnp.zeros((count,), jnp.int32).at[sequence[jnp.where(places < fixed, places, passed)]].set(jnp.asarray(tallies, jnp.int32))

    tallies = jnp.where(number % 4 == 0, named(crowded, number // 4), named(usual, number - number // 4 - 1))
    mixed = jax.random.permutation(jax.random.fold_in(own, 3), count)
    giver, sink = mixed[0:count // 2 * 2:2], mixed[1:count // 2 * 2:2]
    room = jnp.minimum(tallies[giver] - 1, limit - tallies[sink]) // 2
    room = jnp.where((giver == sequence[0]) | (sink == sequence[0]) | (tallies[sink] == 0), 0, jnp.maximum(room, 0))
    passed = jax.random.randint(jax.random.fold_in(own, 4), (count // 2,), 0, 1 << 20) % (room + 1)
    tallies = tallies.at[giver].add(-passed).at[sink].add(passed)
    labels = jnp.searchsorted(jnp.cumsum(tallies), jnp.arange(rows * top), side="right").astype(jnp.int32)
    listing = labels.reshape(top, rows).T
    listing = listing[jax.random.permutation(jax.random.fold_in(own, 1), rows)]
    rotation = jax.random.randint(jax.random.fold_in(own, 2), (rows, 1), 0, top)
    return jnp.take_along_axis(listing, (jnp.arange(top)[None, :] + rotation) % top, axis=1)


def shares(count, total, reach, lean, full):
    weights = [(1 << 20) // math.isqrt(grade ** lean) + 1 for grade in range(1, count + 1)]
    largest = reach if full else min(reach, max(-(-total // count), total * weights[0] // sum(weights)))
    least = 1 if total - largest >= count - 1 else 0
    counts, spare = [largest] + [least] * (count - 1), total - largest - least * (count - 1)
    while spare > 0:
        movable = [i for i in range(1, count) if counts[i] < largest] or [i for i in range(1, count) if counts[i] < reach]
        pool, left = sum([weights[i] for i in movable]), spare
        for i in movable:
            addition = min(reach - counts[i], max(1, left * weights[i] // pool), spare)
            counts[i] = counts[i] + addition
            spare = spare - addition
    return np.array(counts)


def centred(stream_key, dims, deviation, limit, shards=(), held_as=jnp.bfloat16):
    result = deviation * jax.random.normal(stream_key, dims, jnp.float32)
    if shards:
        result = result * block_scale(stream_key, dims, shards, -0.22, 0.18)
    return jnp.clip(result, -limit, limit).astype(held_as)


def setup_inputs(seed: int = 0) -> dict:
    key_list = jax.random.split(jax.random.key(seed), 9)
    field_in = centred(key_list[0], (NC, CL, NRHS), 1.0, 6.0, ((0, 8),))
    left_factors = centred(key_list[1], (NB, CL, RANK), CL ** -0.5, 0.3125, ((0, 32),))
    right_factors = centred(key_list[2], (NB, CL, RANK), (RANK * BPD * N_REP // CPD) ** -0.5, 0.1875, ((0, 32),))
    block_ranks = place_ends(jax.random.randint(key_list[3], (NB,), 8, RANK + 1), jax.random.fold_in(key_list[3], 1), 8, RANK).astype(jnp.int32)
    row_cluster = place_ends(jax.random.randint(key_list[4], (NB,), 0, CPD), jax.random.fold_in(key_list[4], 1), 0, CPD - 1).astype(jnp.int32)
    col_owner_keys = jax.random.split(jax.random.fold_in(key_list[5], 1), NB // BPD)
    col_owner_turns = jax.random.permutation(jax.random.fold_in(key_list[5], 3), NB // BPD)
    col_owner = jax.vmap(lambda own, number: routed_block(jax.random.fold_in(key_list[5], 2), own, number, BPD, OWNERS, 1, MOST, 2))(col_owner_keys, col_owner_turns).reshape((NB, 1))
    col_cluster = place_ends(jax.random.randint(key_list[6], (NB,), 0, CPD), jax.random.fold_in(key_list[6], 1), 0, CPD - 1).astype(jnp.int32)
    near_blocks = centred(key_list[7], (NC, 3, CL, CL), (3 * CL) ** -0.5, 0.1875, ((0, 8), (2, 4)))
    return dict(field_in=field_in, left_factors=left_factors, right_factors=right_factors, block_ranks=block_ranks, row_cluster=row_cluster, col_owner=col_owner, col_cluster=col_cluster, near_blocks=near_blocks)


def reference(field_in, left_factors, right_factors, block_ranks, row_cluster, col_owner, col_cluster, near_blocks):
    groups = N_ROWS * N_REP
    field_wide = field_in.astype(jnp.float32)
    device_ids = jnp.arange(groups, dtype=jnp.int32)
    rows_of = (row_cluster.reshape(groups, BPD) + ((device_ids // N_REP) * CPD)[:, None]).astype(jnp.int32)
    cols_of = (col_owner[:, 0] * CPD + col_cluster).reshape(groups, BPD).astype(jnp.int32)

    def advance(running, items):
        left_part, right_part, ranks_here, rows_here, cols_here = items
        picked = field_wide[rows_here]
        coeffs = jnp.einsum("bcr,bcn->brn", left_part.astype(jnp.float32), picked)
        keeper = jnp.arange(RANK, dtype=jnp.int32)[None, :, None] < ranks_here[:, None, None]
        coeffs = jnp.where(keeper, coeffs, jnp.float32(0.0)).astype(jnp.bfloat16)
        coeffs = lax.optimization_barrier(coeffs).astype(jnp.float32)
        contrib = jnp.einsum("bcr,brn->bcn", right_part.astype(jnp.float32), coeffs).astype(jnp.bfloat16)
        contrib = lax.optimization_barrier(contrib).astype(jnp.float32)
        return running.at[cols_here].add(contrib), None

    start_total = jnp.zeros((CPD * N_ROWS, CL, NRHS), jnp.float32)
    far_field, _ = lax.scan(advance, start_total, (left_factors.reshape(groups, BPD, CL, RANK), right_factors.reshape(groups, BPD, CL, RANK), block_ranks.reshape(groups, BPD), rows_of, cols_of))
    near_wide = near_blocks.astype(jnp.float32)
    terms = [jnp.einsum("cpq,cpn->cqn", near_wide[:, offset], field_wide) for offset in range(3)]
    return far_field + terms[1] + jnp.roll(terms[2], 1, axis=0) + jnp.roll(terms[0], -1, axis=0)
```

```python
import functools

import jax
import jax.numpy as jnp
from jax import lax
from jax.experimental import pallas as pl
from jax.experimental.pallas import tpu as pltpu
from jax.sharding import PartitionSpec as P

MESH = pl.DeviceIdType.MESH
PARTS = 2
BF16 = jnp.bfloat16
F32 = jnp.float32


def dot_rows(left, right):
    return lax.dot_general(left, right, (((0,), (0,)), ((), ())), preferred_element_type=F32)


def kernel(
    owners, reps, most, tab, field, ut, vt, near, out,
    vsend, vrecv, vtr, csend, crecv, hnear, hfield, total, *rest,
):
    stages = reps.bit_length() - 1
    rsend, rrecv = rest[:stages], rest[stages:2 * stages]
    vs, vr, cs, cr, hs, hr, rs, rr, gs, gr = rest[2 * stages:]
    group = owners
    row, rep = lax.axis_index("rows"), lax.axis_index("rep")
    place_in = lax.rem(row, group)
    base = row - place_in
    blocks, rank, width = ut.shape
    clusters, _, columns = field.shape
    share = near.shape[2]
    part = columns // PARTS
    depth = most * rank
    peers = group - 1

    barrier = pltpu.get_barrier_semaphore()

    @pl.loop(1, owners)
    def _(d):
        pl.semaphore_signal(
            barrier, inc=1, device_id=(lax.rem(row + d, owners), rep), device_id_type=MESH
        )

    @pl.loop(1, reps)
    def _(d):
        pl.semaphore_signal(
            barrier, inc=1, device_id=(row, lax.rem(rep + d, reps)), device_id_type=MESH
        )

    def peer(d):
        return base + lax.rem(place_in + d, group)

    def turn(k):
        step = (k + 1) // 2
        return group // 2 + lax.rem(k, 2) * step - (1 - lax.rem(k, 2)) * step

    def v_copy(d):
        return pltpu.make_async_remote_copy(
            src_ref=vsend.at[d], dst_ref=vrecv.at[d], send_sem=vs.at[d], recv_sem=vr.at[d],
            device_id=(peer(d), rep), device_id_type=MESH,
        )

    def c_copy(h, d):
        return pltpu.make_async_remote_copy(
            src_ref=csend.at[h, d], dst_ref=crecv.at[h, d],
            send_sem=cs.at[h, d], recv_sem=cr.at[h, d],
            device_id=(peer(d), rep), device_id_type=MESH,
        )

    def pack(d, target, owner):
        for j in range(most):
            target[d, pl.ds(j * rank, rank), :] = vt[tab[0, owner * most + j]]

    def coeffs(d, target, owner):
        extra = csend.shape[2] - depth
        lines = lax.broadcasted_iota(jnp.int32, (extra, part), 0)
        marks = jnp.full((extra, part), clusters, jnp.int32)
        for j in range(most):
            slot = owner * most + j
            value = jnp.dot(ut[tab[0, slot]], field[tab[1, slot]], preferred_element_type=F32)
            kept = lax.broadcasted_iota(jnp.int32, (rank, columns), 0) < tab[2, slot]
            value = jnp.where(kept, value, 0.0).astype(BF16)
            for h in range(PARTS):
                target[h, d, pl.ds(j * rank, rank), :] = value[:, h * part:(h + 1) * part]
            marks = jnp.where(lines == j, tab[3, slot], marks)
        for h in range(PARTS):
            target[h, d, pl.ds(depth, extra), :] = marks.astype(F32).astype(BF16)

    my_rows = pl.ds(pl.multiple_of(rep * share, share), share)

    def halo_copies():
        made = []
        for side, cluster, offset, shift in ((0, clusters - 1, 2, 1), (1, 0, 0, owners - 1)):
            where = (lax.rem(row + shift, owners), rep)
            made.append(pltpu.make_async_remote_copy(
                src_ref=near.at[cluster, offset], dst_ref=hnear.at[side],
                send_sem=hs.at[2 * side], recv_sem=hr.at[2 * side],
                device_id=where, device_id_type=MESH,
            ))
            made.append(pltpu.make_async_remote_copy(
                src_ref=field.at[cluster, my_rows, :], dst_ref=hfield.at[side],
                send_sem=hs.at[2 * side + 1], recv_sem=hr.at[2 * side + 1],
                device_id=where, device_id_type=MESH,
            ))
        return made

    plan = []
    low, size = 0, clusters
    for t in range(stages):
        bit = lax.rem(rep // (1 << t), 2)
        half = size // 2
        partner = rep + (1 << t) * (1 - 2 * bit)
        plan.append((half, partner, low + bit * half, low + (1 - bit) * half))
        low, size = low + bit * half, half

    def labels_of(source, h, d):
        return jnp.concatenate(
            [
                jnp.broadcast_to(source[h, d, pl.ds(depth + j, 1), :].astype(F32), (rank, part))
                for j in range(most)
            ],
            axis=0,
        ).astype(BF16)

    def part_of(right, source, labels, h, d, c):
        label = jnp.asarray(c, jnp.int32).astype(F32).astype(BF16)
        picked = jnp.where(
            labels == label, source[h, d, pl.ds(0, depth), :], jnp.zeros((), BF16)
        )
        return jnp.dot(right[d], picked, preferred_element_type=F32)

    pl.semaphore_wait(barrier, owners + reps - 2)

    @pl.loop(0, peers)
    def _(k):
        d = turn(k)
        pack(d, vsend, peer(d))
        v_copy(d).start()

    halos = halo_copies()
    for copy in halos:
        copy.start()

    @pl.loop(0, peers)
    def _(k):
        d = turn(k)
        coeffs(d, csend, peer(d))
        c_copy(0, d).start()

    for h in range(1, PARTS):
        @pl.loop(0, peers)
        def _(k):
            c_copy(h, turn(k)).start()

    pack(0, vrecv, row)
    coeffs(0, crecv, row)

    def put(c, value):
        for h in range(PARTS):
            total[h, c] = value[:, h * part:(h + 1) * part]

    def add(c, value):
        for h in range(PARTS):
            total[h, c] = total[h, c] + value[:, h * part:(h + 1) * part]

    @pl.loop(0, clusters)
    def _(c):
        put(c, dot_rows(near[c, 1], field[c, my_rows, :]))

    @pl.loop(0, clusters - 1)
    def _(c):
        add(c + 1, dot_rows(near[c, 2], field[c, my_rows, :]))
        add(c, dot_rows(near[c + 1, 0], field[c + 1, my_rows, :]))

    for copy in halos:
        copy.wait_recv()
    add(0, dot_rows(hnear[0], hfield[0]))
    add(clusters - 1, dot_rows(hnear[1], hfield[1]))

    def far(h, d):
        if h == 0:
            vtr[d] = vrecv[d].T
        labels = labels_of(crecv, h, d)

        @pl.loop(0, clusters)
        def _(c):
            total[h, c] = total[h, c] + part_of(vtr, crecv, labels, h, d, c)

    def far_span(h, first, last):
        @pl.loop(first, last)
        def _(k):
            d = turn(peers - 1 - k)
            if h == 0:
                v_copy(d).wait_recv()
            c_copy(h, d).wait_recv()
            far(h, d)

    def r_copy(h, t):
        return pltpu.make_async_remote_copy(
            src_ref=rsend[t].at[h], dst_ref=rrecv[t].at[h],
            send_sem=rs.at[h, t], recv_sem=rr.at[h, t],
            device_id=(row, plan[t][1]), device_id_type=MESH,
        )

    def g_copy(h, t):
        half, partner, keep, _ = plan[t]
        block = out.at[pl.ds(keep, half), :, pl.ds(h * part, part)]
        return pltpu.make_async_remote_copy(
            src_ref=block, dst_ref=block, send_sem=gs.at[h, t], recv_sem=gr.at[h, t],
            device_id=(row, partner), device_id_type=MESH,
        )

    def give(h, t):
        half, _, _, away = plan[t]

        @pl.loop(0, half)
        def _(i):
            rsend[t][h, i] = total[h, away + i].astype(rsend[t].dtype)

        r_copy(h, t).start()

    def take(h, t):
        half, _, keep, _ = plan[t]
        r_copy(h, t).wait_recv()

        @pl.loop(0, half)
        def _(i):
            value = total[h, keep + i] + rrecv[t][h, i].astype(F32)
            if t == stages - 1:
                out[keep + i, :, pl.ds(h * part, part)] = value.astype(BF16)
            else:
                total[h, keep + i] = value

    def sequence(h):
        steps = [lambda: give(h, 0)]
        for t in range(stages):
            if t < stages - 1:
                steps.append(lambda t=t: (take(h, t), give(h, t + 1)))
            else:
                steps.append(lambda t=t: (take(h, t), g_copy(h, t).start()))
        for t in range(stages - 1, 0, -1):
            steps.append(lambda t=t: (g_copy(h, t).wait_recv(), g_copy(h, t - 1).start()))
        steps.append(lambda: g_copy(h, 0).wait_recv())
        return steps

    ahead, behind = sequence(0), sequence(1)
    far(0, 0)
    far_span(0, 0, peers)
    ahead[0]()
    for step in ahead[1:stages]:
        step()
    middle = peers // 2
    far(1, 0)
    far_span(1, 0, middle)
    ahead[stages]()
    far_span(1, middle, peers)
    behind[0]()
    later = ahead[stages + 1:]
    for place, step in enumerate(behind[1:]):
        if place < len(later):
            later[place]()
        step()

    @pl.loop(1, group)
    def _(d):
        v_copy(d).wait_send()
        for h in range(PARTS):
            c_copy(h, d).wait_send()

    for copy in halos:
        copy.wait_send()
    for h in range(PARTS):
        for t in range(stages):
            r_copy(h, t).wait_send()
            g_copy(h, t).wait_send()


def cube(
    most, tab, rowc, ranks, field, ut, vt, near, out,
    cnat, vsend, csend, vcat, ccat, vtr, labels, hnear, hfield, total, acc,
    ksend, krecv, qrecv, gsend, grecv, ysend, yrecv, zsend, zrecv,
    xsend, xrecv, fsend, frecv,
    vs, vr, cs, cr, hs, hr, ks, kr, qs, qr, gs, gr, ys, yr, zs, zr, xs, xr, fs, fr, os, orr,
):
    owners, reps = lax.axis_size("rows"), lax.axis_size("rep")
    row, rep = lax.axis_index("rows"), lax.axis_index("rep")
    half = owners // 2
    w, u, y = row // half, lax.rem(row // 2, 2), lax.rem(row, 2)
    x, core = rep // 2, lax.rem(rep, 2)
    blocks, rank, width = ut.shape
    clusters, _, columns = field.shape
    share = near.shape[2]
    depth = most * rank
    pad = csend.shape[1] - depth
    quad = clusters // 2
    pair = clusters // 4

    def at(w_, u_, y_):
        return w_ * half + u_ * 2 + y_

    def mix(t, one, two):
        return one * (1 - t) + two * t

    to_y = (at(w, u, 1 - y), rep)
    to_z = (at(w, 1 - u, y), rep)
    to_x = (row, (1 - x) * 2 + core)
    to_core = (row, x * 2 + 1 - core)
    to_across = (at(1 - w, u, mix(u, y, x)), mix(u, x, y) * 2 + core)
    after = (lax.rem(row + 1, owners), rep)
    before = (lax.rem(row + owners - 1, owners), rep)
    partners = (to_y, to_z, to_x, to_core, to_across, after, before)

    sends = (
        (to_y, at(1 - w, 0, 1 - y)),
        (to_x, at(1 - w, 1, 1 - x)),
        (to_z, at(w, 1 - u, 1 - y)),
        (to_z, at(w, 1 - u, y)),
    )
    owns = (at(1 - w, 0, y), at(1 - w, 1, x), at(w, u, 1 - y), row)
    bits = (x, y, x, x)
    mine = core * quad
    theirs = (1 - core) * quad

    def remote(src, dst, send, recv, where):
        return pltpu.make_async_remote_copy(
            src_ref=src, dst_ref=dst, send_sem=send, recv_sem=recv,
            device_id=where, device_id_type=MESH,
        )

    def v_copy(i):
        return remote(vsend.at[i], vcat.at[i, pl.ds(depth, depth)], vs.at[i], vr.at[i], sends[i][0])

    def c_copy(i):
        spot = pl.ds(pad + depth, depth + pad)
        return remote(csend.at[i], ccat.at[i, spot], cs.at[i], cr.at[i], sends[i][0])

    def k_copy(i, n):
        return remote(ksend.at[i, n], krecv.at[i, n], ks.at[i, n], kr.at[i, n], to_core)

    def q_copy(n):
        return remote(total.at[theirs + n], qrecv.at[n], qs.at[n], qr.at[n], to_core)

    def g_copy(i, m):
        where = (to_x, to_y)[i]
        return remote(gsend.at[i, m], grecv.at[i, m], gs.at[i, m], gr.at[i, m], where)

    def y_copy(n):
        return remote(ysend.at[n], yrecv.at[n], ys.at[n], yr.at[n], to_y)

    def z_copy(m):
        return remote(zsend.at[m], zrecv.at[m], zs.at[m], zr.at[m], to_z)

    def x_copy(m):
        return remote(xsend.at[m], xrecv.at[m], xs.at[m], xr.at[m], to_across)

    def f_copy(m):
        return remote(fsend.at[m], frecv.at[m], fs.at[m], fr.at[m], to_x)

    def o_copy(m):
        block = out.at[mine + x * pair + m]
        return remote(block, block, os.at[m], orr.at[m], to_x)

    def p_copy(n):
        block = out.at[mine + n]
        return remote(block, block, os.at[pair + n], orr.at[pair + n], to_core)

    barrier = pltpu.get_barrier_semaphore()
    for where in partners:
        pl.semaphore_signal(barrier, inc=1, device_id=where, device_id_type=MESH)

    def pack_v(owner, put):
        for j in range(most):
            put(j * rank, vt[tab[0, owner * most + j]])

    def pack_c(owner, put, put_marks):
        lines = lax.broadcasted_iota(jnp.int32, (pad, columns), 0)
        marks = jnp.full((pad, columns), clusters, jnp.int32)
        for j in range(most):
            slot = owner * most + j
            put(j * rank, cnat[tab[0, slot]])
            marks = jnp.where(lines == j, tab[1, slot], marks)
        put_marks(marks.astype(F32).astype(BF16))

    def send_v(i):
        def put(spot, value):
            vsend[i, pl.ds(spot, rank), :] = value

        pack_v(sends[i][1], put)

    def send_c(i):
        def put(spot, value):
            csend[i, pl.ds(spot, rank), :] = value

        def put_marks(value):
            csend[i, pl.ds(depth, pad), :] = value

        pack_c(sends[i][1], put, put_marks)
        c_copy(i).start()

    def own(i):
        def put_v(spot, value):
            vcat[i, pl.ds(spot, rank), :] = value

        def put_c(spot, value):
            ccat[i, pl.ds(pad + spot, rank), :] = value

        def put_marks(value):
            ccat[i, pl.ds(0, pad), :] = value

        pack_v(owns[i], put_v)
        pack_c(owns[i], put_c, put_marks)

    for i in range(4):
        send_v(i)
    pl.semaphore_wait(barrier, len(partners))
    for i in range(3):
        v_copy(i).start()

    @pl.loop(0, blocks)
    def _(b):
        value = jnp.dot(ut[b], field[rowc[b]], preferred_element_type=F32)
        kept = lax.broadcasted_iota(jnp.int32, (rank, columns), 0) < ranks[b]
        cnat[b] = jnp.where(kept, value, 0.0).astype(BF16)

    for i in range(3):
        send_c(i)
    v_copy(3).start()
    send_c(3)

    my_rows = pl.ds(pl.multiple_of(rep * share, share), share)
    halos = []
    for side, cluster, offset, where in ((0, clusters - 1, 2, after), (1, 0, 0, before)):
        halos.append(remote(
            near.at[cluster, offset], hnear.at[side], hs.at[2 * side], hr.at[2 * side], where
        ))
        halos.append(remote(
            field.at[cluster, my_rows, :], hfield.at[side],
            hs.at[2 * side + 1], hr.at[2 * side + 1], where,
        ))
    for copy in halos:
        copy.start()

    for i in range(4):
        own(i)

    def close(c, offset):
        return dot_rows(near[c, offset], field[c, my_rows, :])

    @pl.loop(1, clusters - 1)
    def _(c):
        total[c] = close(c, 1) + close(c - 1, 2) + close(c + 1, 0)

    last = clusters - 1
    total[0] = close(0, 1) + close(1, 0)
    total[last] = close(last, 1) + close(last - 1, 2)

    def label_rows(i, start, spot):
        for j in range(most):
            line = ccat[i, pl.ds(start + j, 1), :].astype(F32)
            labels[pl.ds(spot + j * rank, rank), :] = (
                jnp.broadcast_to(line, (rank, columns)).astype(BF16)
            )

    def part_of(i, c):
        label = jnp.asarray(c, jnp.int32).astype(F32).astype(BF16)
        picked = jnp.where(
            labels[...] == label, ccat[i, pl.ds(pad, 2 * depth), :], jnp.zeros((), BF16)
        )
        return jnp.dot(vtr[...], picked, preferred_element_type=F32)

    def turn(i, k):
        side = mix(k // pair, 1 - bits[i], bits[i])
        return side * pair + lax.rem(k, pair)

    def partial(i):
        label_rows(i, 0, 0)
        v_copy(i).wait_recv()
        vtr[...] = vcat[i].T
        c_copy(i).wait_recv()
        label_rows(i, pad + 2 * depth, depth)

        @pl.loop(0, quad)
        def _(k):
            n = turn(i, k)
            value = part_of(i, theirs + n)
            if i < 3:
                ksend[i, n] = value.astype(BF16)
                k_copy(i, n).start()
            else:
                total[theirs + n] = total[theirs + n] + value
                q_copy(n).start()

        @pl.loop(0, quad)
        def _(k):
            n = turn(i, k)
            value = part_of(i, mine + n)
            if i < 3:
                acc[i, n] = value
            else:
                total[mine + n] = total[mine + n] + value

    def give_g(i):
        @pl.loop(0, pair)
        def _(m):
            n = (1 - bits[i]) * pair + m
            k_copy(i, n).wait_recv()
            gsend[i, m] = (acc[i, n] + krecv[i, n].astype(F32)).astype(BF16)
            g_copy(i, m).start()

        @pl.loop(0, pair)
        def _(m):
            n = bits[i] * pair + m
            k_copy(i, n).wait_recv()
            acc[i, n] = acc[i, n] + krecv[i, n].astype(F32)

    partial(0)
    partial(1)
    give_g(0)
    partial(2)
    give_g(1)

    @pl.loop(0, quad)
    def _(k):
        n = turn(2, k)
        k_copy(2, n).wait_recv()
        ysend[n] = (acc[2, n] + krecv[2, n].astype(F32)).astype(BF16)
        y_copy(n).start()

    for copy in halos:
        copy.wait_recv()
    total[0] = total[0] + dot_rows(hnear[0], hfield[0])
    total[last] = total[last] + dot_rows(hnear[1], hfield[1])
    partial(3)

    @pl.loop(0, pair)
    def _(m):
        for i in range(2):
            g_copy(i, m).wait_recv()
            n = bits[i] * pair + m
            acc[i, n] = acc[i, n] + grecv[i, m].astype(F32)
        zsend[m] = acc[1 - u, mix(1 - u, x, y) * pair + m].astype(BF16)
        z_copy(m).start()

    @pl.loop(0, pair)
    def _(m):
        z_copy(m).wait_recv()
        value = acc[u, mix(u, x, y) * pair + m] + zrecv[m].astype(F32)
        xsend[m] = value.astype(BF16)
        x_copy(m).start()

    @pl.loop(0, pair)
    def _(m):
        n = (1 - x) * pair + m
        q_copy(n).wait_recv()
        y_copy(n).wait_recv()
        fsend[m] = (total[mine + n] + qrecv[n] + yrecv[n].astype(F32)).astype(BF16)
        f_copy(m).start()

    @pl.loop(0, pair)
    def _(m):
        n = x * pair + m
        q_copy(n).wait_recv()
        y_copy(n).wait_recv()
        value = total[mine + n] + qrecv[n] + yrecv[n].astype(F32)
        f_copy(m).wait_recv()
        value = value + frecv[m].astype(F32)
        x_copy(m).wait_recv()
        out[mine + n] = (value + xrecv[m].astype(F32)).astype(BF16)
        o_copy(m).start()
        p_copy(n).start()

    @pl.loop(0, pair)
    def _(m):
        o_copy(m).wait_recv()
        p_copy((1 - x) * pair + m).start()

    @pl.loop(0, quad)
    def _(n):
        p_copy(n).wait_recv()

    for copy in halos:
        copy.wait_send()
    for i in range(4):
        v_copy(i).wait_send()
        c_copy(i).wait_send()

    @pl.loop(0, quad)
    def _(n):
        for i in range(3):
            k_copy(i, n).wait_send()
        q_copy(n).wait_send()
        y_copy(n).wait_send()
        p_copy(n).wait_send()

    @pl.loop(0, pair)
    def _(m):
        for i in range(2):
            g_copy(i, m).wait_send()
        z_copy(m).wait_send()
        x_copy(m).wait_send()
        f_copy(m).wait_send()
        o_copy(m).wait_send()


def slots_of(col_owner, owners, most):
    target = col_owner[:, 0]
    number = jnp.arange(target.shape[0], dtype=jnp.int32)
    same = (target[:, None] == target[None, :]) & (number[None, :] < number[:, None])
    slot = target * most + jnp.sum(same.astype(jnp.int32), axis=1)
    return slot[:, None] == jnp.arange(owners * most, dtype=jnp.int32)[None, :]


def table(held, clusters, facts):
    lift = [0] * (len(facts) - 1) + [clusters]
    tab = jnp.sum(jnp.where(held[None], jnp.stack(facts)[:, :, None], 0), axis=1)
    return tab + jnp.array(lift, jnp.int32)[:, None]


def shards(
    field_in,
    left_factors,
    right_factors,
    block_ranks,
    row_cluster,
    col_owner,
    col_cluster,
    near_blocks,
):
    owners, reps = lax.axis_size("rows"), lax.axis_size("rep")
    blocks, width, rank = left_factors.shape
    clusters, _, columns = field_in.shape
    share = near_blocks.shape[2]
    most = 5 * blocks // (4 * owners) + 1
    part = columns // PARTS
    depth = most * rank
    pad = -(-most // 16) * 16
    tall = depth + pad
    stages = reps.bit_length() - 1

    held = slots_of(col_owner, owners, most)
    number = jnp.arange(blocks, dtype=jnp.int32)
    smem = pl.BlockSpec(memory_space=pltpu.SMEM)
    vmem = pl.BlockSpec(memory_space=pltpu.VMEM)
    dma = pltpu.SemaphoreType.DMA
    arrays = (
        field_in,
        jnp.swapaxes(left_factors, 1, 2),
        jnp.swapaxes(right_factors, 1, 2),
        near_blocks,
    )
    cubic = stages == 2 and owners == 2 ** 3
    if cubic:
        quad, pair = clusters // 2, clusters // 4
        slab = (width, columns)
        gathered = pl.pallas_call(
            functools.partial(cube, most),
            out_shape=jax.ShapeDtypeStruct(field_in.shape, BF16),
            in_specs=[smem] * 3 + [vmem] * 4,
            out_specs=vmem,
            scratch_shapes=[
                pltpu.VMEM((blocks, rank, columns), BF16),
                pltpu.VMEM((4, depth, width), BF16),
                pltpu.VMEM((4, tall, columns), BF16),
                pltpu.VMEM((4, 2 * depth, width), BF16),
                pltpu.VMEM((4, 2 * tall, columns), BF16),
                pltpu.VMEM((width, 2 * depth), BF16),
                pltpu.VMEM((2 * depth, columns), BF16),
                pltpu.VMEM((2, share, width), BF16),
                pltpu.VMEM((2, share, columns), BF16),
                pltpu.VMEM((clusters, *slab), F32),
                pltpu.VMEM((3, quad, *slab), F32),
                pltpu.VMEM((3, quad, *slab), BF16),
                pltpu.VMEM((3, quad, *slab), BF16),
                pltpu.VMEM((quad, *slab), F32),
                pltpu.VMEM((2, pair, *slab), BF16),
                pltpu.VMEM((2, pair, *slab), BF16),
                pltpu.VMEM((quad, *slab), BF16),
                pltpu.VMEM((quad, *slab), BF16),
                *[pltpu.VMEM((pair, *slab), BF16)] * 6,
                *[dma((4,))] * 6,
                *[dma((3, quad))] * 2,
                *[dma((quad,))] * 2,
                *[dma((2, pair))] * 2,
                *[dma((quad,))] * 2,
                *[dma((pair,))] * 6,
                *[dma((pair + quad,))] * 2,
            ],
            compiler_params=pltpu.CompilerParams(
                collective_id=0, has_side_effects=True, vmem_limit_bytes=60 * 1024 * 1024
            ),
        )(table(held, clusters, [number, col_cluster - clusters]), row_cluster, block_ranks, *arrays)
        return gathered.astype(F32)

    halves = [clusters >> (t + 1) for t in range(stages)]
    steps = [
        pltpu.VMEM((PARTS, half, width, part), BF16 if t else F32) for t, half in enumerate(halves)
    ]
    gathered = pl.pallas_call(
        functools.partial(kernel, owners, reps, most),
        out_shape=jax.ShapeDtypeStruct(field_in.shape, BF16),
        in_specs=[smem] + [vmem] * 4,
        out_specs=vmem,
        scratch_shapes=[
            pltpu.VMEM((owners, depth, width), BF16),
            pltpu.VMEM((owners, depth, width), BF16),
            pltpu.VMEM((owners, width, depth), BF16),
            pltpu.VMEM((PARTS, owners, tall, part), BF16),
            pltpu.VMEM((PARTS, owners, tall, part), BF16),
            pltpu.VMEM((2, share, width), BF16),
            pltpu.VMEM((2, share, columns), BF16),
            pltpu.VMEM((PARTS, clusters, width, part), F32),
            *steps,
            *steps,
            dma((owners,)),
            dma((owners,)),
            dma((PARTS, owners)),
            dma((PARTS, owners)),
            dma((4,)),
            dma((4,)),
            *[dma((PARTS, stages))] * 4,
        ],
        compiler_params=pltpu.CompilerParams(
            collective_id=0, has_side_effects=True, vmem_limit_bytes=60 * 1024 * 1024
        ),
    )(table(held, clusters, [number, row_cluster, block_ranks, col_cluster - clusters]), *arrays)
    return gathered.astype(F32)


def solution(mesh):
    in_specs = (
        P("rows", None, None),
        P(("rows", "rep"), None, None),
        P(("rows", "rep"), None, None),
        P(("rows", "rep")),
        P(("rows", "rep")),
        P(("rows", "rep"), None),
        P(("rows", "rep")),
        P("rows", None, "rep", None),
    )
    out_specs = P("rows", None, None)
    return jax.shard_map(shards, mesh=mesh, in_specs=in_specs, out_specs=out_specs, check_vma=False)
```

```python
import functools

import jax
import jax.numpy as jnp
from jax import lax
from jax.experimental import pallas as pl
from jax.experimental.pallas import tpu as pltpu
from jax.sharding import PartitionSpec as P

MESH = pl.DeviceIdType.MESH
PARTS = 2
SPLIT = 2
BF16 = jnp.bfloat16
F32 = jnp.float32


def dot_rows(left, right):
    return lax.dot_general(left, right, (((0,), (0,)), ((), ())), preferred_element_type=F32)


def kernel(
    owners, reps, most, tab, field, ut, vt, near, out,
    vsend, vrecv, vtr, csend, crecv, hnear, hfield, total, *rest,
):
    stages = reps.bit_length() - 1
    rsend, rrecv = rest[:stages], rest[stages:2 * stages]
    vs, vr, cs, cr, hs, hr, rs, rr, gs, gr = rest[2 * stages:]
    group = owners
    row, rep = lax.axis_index("rows"), lax.axis_index("rep")
    place_in = lax.rem(row, group)
    base = row - place_in
    blocks, rank, width = ut.shape
    clusters, _, columns = field.shape
    share = near.shape[2]
    part = columns // PARTS
    depth = most * rank
    peers = group - 1

    barrier = pltpu.get_barrier_semaphore()

    @pl.loop(1, owners)
    def _(d):
        pl.semaphore_signal(
            barrier, inc=1, device_id=(lax.rem(row + d, owners), rep), device_id_type=MESH
        )

    @pl.loop(1, reps)
    def _(d):
        pl.semaphore_signal(
            barrier, inc=1, device_id=(row, lax.rem(rep + d, reps)), device_id_type=MESH
        )

    def peer(d):
        return base + lax.rem(place_in + d, group)

    def turn(k):
        step = (k + 1) // 2
        return group // 2 + lax.rem(k, 2) * step - (1 - lax.rem(k, 2)) * step

    def v_copy(d):
        return pltpu.make_async_remote_copy(
            src_ref=vsend.at[d], dst_ref=vrecv.at[d], send_sem=vs.at[d], recv_sem=vr.at[d],
            device_id=(peer(d), rep), device_id_type=MESH,
        )

    def c_copy(h, d):
        return pltpu.make_async_remote_copy(
            src_ref=csend.at[h, d], dst_ref=crecv.at[h, d],
            send_sem=cs.at[h, d], recv_sem=cr.at[h, d],
            device_id=(peer(d), rep), device_id_type=MESH,
        )

    def pack(d, target, owner):
        for j in range(most):
            target[d, pl.ds(j * rank, rank), :] = vt[tab[0, owner * most + j]]

    def coeffs(d, target, owner):
        extra = csend.shape[2] - depth
        lines = lax.broadcasted_iota(jnp.int32, (extra, part), 0)
        marks = jnp.full((extra, part), clusters, jnp.int32)
        for j in range(most):
            slot = owner * most + j
            value = jnp.dot(ut[tab[0, slot]], field[tab[1, slot]], preferred_element_type=F32)
            kept = lax.broadcasted_iota(jnp.int32, (rank, columns), 0) < tab[2, slot]
            value = jnp.where(kept, value, 0.0).astype(BF16)
            for h in range(PARTS):
                target[h, d, pl.ds(j * rank, rank), :] = value[:, h * part:(h + 1) * part]
            marks = jnp.where(lines == j, tab[3, slot], marks)
        for h in range(PARTS):
            target[h, d, pl.ds(depth, extra), :] = marks.astype(F32).astype(BF16)

    my_rows = pl.ds(pl.multiple_of(rep * share, share), share)

    def halo_copies():
        made = []
        for side, cluster, offset, shift in ((0, clusters - 1, 2, 1), (1, 0, 0, owners - 1)):
            where = (lax.rem(row + shift, owners), rep)
            made.append(pltpu.make_async_remote_copy(
                src_ref=near.at[cluster, offset], dst_ref=hnear.at[side],
                send_sem=hs.at[2 * side], recv_sem=hr.at[2 * side],
                device_id=where, device_id_type=MESH,
            ))
            made.append(pltpu.make_async_remote_copy(
                src_ref=field.at[cluster, my_rows, :], dst_ref=hfield.at[side],
                send_sem=hs.at[2 * side + 1], recv_sem=hr.at[2 * side + 1],
                device_id=where, device_id_type=MESH,
            ))
        return made

    plan = []
    low, size = 0, clusters
    for t in range(stages):
        bit = lax.rem(rep // (1 << t), 2)
        half = size // 2
        partner = rep + (1 << t) * (1 - 2 * bit)
        plan.append((half, partner, low + bit * half, low + (1 - bit) * half))
        low, size = low + bit * half, half

    def labels_of(source, h, d):
        return jnp.concatenate(
            [
                jnp.broadcast_to(source[h, d, pl.ds(depth + j, 1), :].astype(F32), (rank, part))
                for j in range(most)
            ],
            axis=0,
        ).astype(BF16)

    def part_of(right, source, labels, h, d, c):
        label = jnp.asarray(c, jnp.int32).astype(F32).astype(BF16)
        picked = jnp.where(
            labels == label, source[h, d, pl.ds(0, depth), :], jnp.zeros((), BF16)
        )
        return jnp.dot(right[d], picked, preferred_element_type=F32)

    pl.semaphore_wait(barrier, owners + reps - 2)

    @pl.loop(0, peers)
    def _(k):
        d = turn(k)
        pack(d, vsend, peer(d))
        v_copy(d).start()

    halos = halo_copies()
    for copy in halos:
        copy.start()

    @pl.loop(0, peers)
    def _(k):
        d = turn(k)
        coeffs(d, csend, peer(d))
        c_copy(0, d).start()

    for h in range(1, PARTS):
        @pl.loop(0, peers)
        def _(k):
            c_copy(h, turn(k)).start()

    pack(0, vrecv, row)
    coeffs(0, crecv, row)

    def put(c, value):
        for h in range(PARTS):
            total[h, c] = value[:, h * part:(h + 1) * part]

    def add(c, value):
        for h in range(PARTS):
            total[h, c] = total[h, c] + value[:, h * part:(h + 1) * part]

    @pl.loop(0, clusters)
    def _(c):
        put(c, dot_rows(near[c, 1], field[c, my_rows, :]))

    @pl.loop(0, clusters - 1)
    def _(c):
        add(c + 1, dot_rows(near[c, 2], field[c, my_rows, :]))
        add(c, dot_rows(near[c + 1, 0], field[c + 1, my_rows, :]))

    for copy in halos:
        copy.wait_recv()
    add(0, dot_rows(hnear[0], hfield[0]))
    add(clusters - 1, dot_rows(hnear[1], hfield[1]))

    def far(h, d):
        if h == 0:
            vtr[d] = vrecv[d].T
        labels = labels_of(crecv, h, d)

        @pl.loop(0, clusters)
        def _(c):
            total[h, c] = total[h, c] + part_of(vtr, crecv, labels, h, d, c)

    def far_span(h, first, last):
        @pl.loop(first, last)
        def _(k):
            d = turn(peers - 1 - k)
            if h == 0:
                v_copy(d).wait_recv()
            c_copy(h, d).wait_recv()
            far(h, d)

    def r_copy(h, t):
        return pltpu.make_async_remote_copy(
            src_ref=rsend[t].at[h], dst_ref=rrecv[t].at[h],
            send_sem=rs.at[h, t], recv_sem=rr.at[h, t],
            device_id=(row, plan[t][1]), device_id_type=MESH,
        )

    def g_copy(h, t):
        half, partner, keep, _ = plan[t]
        block = out.at[pl.ds(keep, half), :, pl.ds(h * part, part)]
        return pltpu.make_async_remote_copy(
            src_ref=block, dst_ref=block, send_sem=gs.at[h, t], recv_sem=gr.at[h, t],
            device_id=(row, partner), device_id_type=MESH,
        )

    def give(h, t):
        half, _, _, away = plan[t]

        @pl.loop(0, half)
        def _(i):
            rsend[t][h, i] = total[h, away + i].astype(rsend[t].dtype)

        r_copy(h, t).start()

    def take(h, t):
        half, _, keep, _ = plan[t]
        r_copy(h, t).wait_recv()

        @pl.loop(0, half)
        def _(i):
            value = total[h, keep + i] + rrecv[t][h, i].astype(F32)
            if t == stages - 1:
                out[keep + i, :, pl.ds(h * part, part)] = value.astype(BF16)
            else:
                total[h, keep + i] = value

    def sequence(h):
        steps = [lambda: give(h, 0)]
        for t in range(stages):
            if t < stages - 1:
                steps.append(lambda t=t: (take(h, t), give(h, t + 1)))
            else:
                steps.append(lambda t=t: (take(h, t), g_copy(h, t).start()))
        for t in range(stages - 1, 0, -1):
            steps.append(lambda t=t: (g_copy(h, t).wait_recv(), g_copy(h, t - 1).start()))
        steps.append(lambda: g_copy(h, 0).wait_recv())
        return steps

    ahead, behind = sequence(0), sequence(1)
    far(0, 0)
    far_span(0, 0, peers)
    ahead[0]()
    for step in ahead[1:stages]:
        step()
    middle = peers // 2
    far(1, 0)
    far_span(1, 0, middle)
    ahead[stages]()
    far_span(1, middle, peers)
    behind[0]()
    later = ahead[stages + 1:]
    for place, step in enumerate(behind[1:]):
        if place < len(later):
            later[place]()
        step()

    @pl.loop(1, group)
    def _(d):
        v_copy(d).wait_send()
        for h in range(PARTS):
            c_copy(h, d).wait_send()

    for copy in halos:
        copy.wait_send()
    for h in range(PARTS):
        for t in range(stages):
            r_copy(h, t).wait_send()
            g_copy(h, t).wait_send()


def cube(
    most, rowc, ranks, tab, field_hbm, ut_hbm, vt_hbm, near_hbm, out,
    field, ut, vt, near,
    cnat, vsend, csend, vrecv, crecv, vown, cown, vtr, labels, hnear, hfield, total, acc,
    ksend, krecv, qrecv, gsend, grecv, ysend, yrecv, zsend, zrecv,
    xsend, xrecv, fsend, frecv,
    ins, vs, vr, cs, cr, hs, hr, ks, kr, qs, qr, gs, gr, ys, yr, zs, zr, xs, xr, fs, fr, os, orr,
):
    owners, reps = lax.axis_size("rows"), lax.axis_size("rep")
    row, rep = lax.axis_index("rows"), lax.axis_index("rep")
    half = owners // 2
    w, u, y = row // half, lax.rem(row // 2, 2), lax.rem(row, 2)
    x, core = rep // 2, lax.rem(rep, 2)
    blocks, rank, width = ut.shape
    clusters, _, columns = field.shape
    share = near.shape[2]
    depth = most * rank
    pad = vsend.shape[1] - depth
    quad = clusters // 2
    pair = clusters // 4
    sub = width // SPLIT
    bits_of = (blocks - 1).bit_length()

    def at(w_, u_, y_):
        return w_ * half + u_ * 2 + y_

    def mix(t, one, two):
        return one * (1 - t) + two * t

    to_y = (at(w, u, 1 - y), rep)
    to_z = (at(w, 1 - u, y), rep)
    to_x = (row, (1 - x) * 2 + core)
    to_core = (row, x * 2 + 1 - core)
    to_across = (at(1 - w, u, mix(u, y, x)), mix(u, x, y) * 2 + core)
    to_next = (lax.rem(row + mix(y, owners - 2, 2), owners), rep)
    to_prior = (lax.rem(row + mix(y, 2, owners - 2), owners), rep)
    partners = (to_y, to_z, to_x, to_core, to_across, to_next, to_prior)

    barrier = pltpu.get_barrier_semaphore()
    for where in partners:
        pl.semaphore_signal(barrier, inc=1, device_id=where, device_id_type=MESH)

    loads = [
        pltpu.make_async_copy(src, dst, ins.at[i])
        for i, (src, dst) in enumerate(
            ((vt_hbm, vt), (ut_hbm, ut), (field_hbm, field), (near_hbm, near))
        )
    ]
    for load in loads:
        load.start()

    sends = (
        (to_y, at(1 - w, 0, 1 - y)),
        (to_x, at(1 - w, 1, 1 - x)),
        (to_z, at(w, 1 - u, 1 - y)),
        (to_z, at(w, 1 - u, y)),
    )
    owns = (at(1 - w, 0, y), at(1 - w, 1, x), at(w, u, 1 - y), row)
    bits = (x, y, x, x)
    mine = core * quad
    theirs = (1 - core) * quad

    def remote(src, dst, send, recv, where):
        return pltpu.make_async_remote_copy(
            src_ref=src, dst_ref=dst, send_sem=send, recv_sem=recv,
            device_id=where, device_id_type=MESH,
        )

    def v_copy(i):
        return remote(vsend.at[i], vrecv.at[i], vs.at[i], vr.at[i], sends[i][0])

    def c_copy(i):
        return remote(csend.at[i], crecv.at[i], cs.at[i], cr.at[i], sends[i][0])

    def k_copy(i, n):
        return remote(ksend.at[i, n], krecv.at[i, n], ks.at[i, n], kr.at[i, n], to_core)

    def q_copy(n):
        return remote(total.at[theirs + n], qrecv.at[n], qs.at[n], qr.at[n], to_core)

    def g_copy(i, m):
        where = (to_x, to_y)[i]
        return remote(gsend.at[i, m], grecv.at[i, m], gs.at[i, m], gr.at[i, m], where)

    def y_copy(n):
        return remote(ysend.at[n], yrecv.at[n], ys.at[n], yr.at[n], to_y)

    def z_copy(m):
        return remote(zsend.at[m], zrecv.at[m], zs.at[m], zr.at[m], to_z)

    def x_copy(m):
        return remote(xsend.at[m], xrecv.at[m], xs.at[m], xr.at[m], to_across)

    def f_copy(m):
        return remote(fsend.at[m], frecv.at[m], fs.at[m], fr.at[m], to_x)

    def o_copy(m):
        block = out.at[(mine + x * pair) * SPLIT + m]
        return remote(block, block, os.at[m], orr.at[m], to_x)

    def p_copy(n):
        block = out.at[mine * SPLIT + n]
        spot = pair * SPLIT + n
        return remote(block, block, os.at[spot], orr.at[spot], to_core)

    def pack_v(owner, put):
        lines = lax.broadcasted_iota(jnp.int32, (pad, width), 0)
        marks = jnp.full((pad, width), clusters, jnp.int32)
        for j in range(most):
            put(pl.ds(j * rank, rank), vt[tab[0, owner * most + j]])
            label = tab[1, owner * most + j]
            marks = jnp.where(lines == j, label, marks)
        put(pl.ds(depth, pad), marks.astype(F32).astype(BF16))

    def pack_c(owner, put):
        for j in range(most):
            put(pl.ds(j * rank, rank), cnat[tab[0, owner * most + j]])

    def send_v(i):
        def put(spot, value):
            vsend[i, spot, :] = value

        pack_v(sends[i][1], put)

    def send_c(i):
        def put(spot, value):
            csend[i, spot, :] = value

        pack_c(sends[i][1], put)
        c_copy(i).start()

    my_rows = pl.ds(pl.multiple_of(rep * share, share), share)
    last = clusters - 1
    halos = [
        remote(near.at[y * last, y * 2], hnear, hs.at[0], hr.at[0], to_next),
        remote(field.at[y * last, my_rows, :], hfield, hs.at[1], hr.at[1], to_next),
    ]

    loads[0].wait()
    for i in range(4):
        send_v(i)
    for load in loads[1:]:
        load.wait()
    pl.semaphore_wait(barrier, len(partners))
    for i in range(2):
        v_copy(i).start()
    for copy in halos:
        copy.start()
    v_copy(2).start()

    def coefficients(b):
        value = jnp.dot(ut[b], field[rowc[b]], preferred_element_type=F32)
        kept = lax.broadcasted_iota(jnp.int32, (rank, columns), 0) < ranks[b]
        cnat[b] = jnp.where(kept, value, 0.0).astype(BF16)

    @pl.loop(0, blocks // 4)
    def _(b):
        for e in range(4):
            coefficients(b * 4 + e)

    for i in range(3):
        send_c(i)
    v_copy(3).start()
    send_c(3)

    def cut(value):
        return [value[s * sub:(s + 1) * sub] for s in range(SPLIT)]

    def prepare(d, factors):
        vtr[d] = factors[pl.ds(0, depth), :].T
        for j in range(most):
            line = factors[pl.ds(depth + j, 1), pl.ds(0, columns)].astype(F32)
            labels[d, pl.ds(j * rank, rank), :] = (
                jnp.broadcast_to(line, (rank, columns)).astype(BF16)
            )

    def part_of(d, coeffs, c):
        label = jnp.asarray(c, jnp.int32).astype(F32).astype(BF16)
        picked = jnp.where(labels[d] == label, coeffs[...], jnp.zeros((), BF16))
        return jnp.dot(vtr[d], picked, preferred_element_type=F32)

    def own(i):
        def put_v(spot, value):
            vown[spot, :] = value

        def put_c(spot, value):
            cown[spot, :] = value

        pack_v(owns[i], put_v)
        pack_c(owns[i], put_c)
        prepare(3, vown)

        @pl.loop(0, clusters // 2)
        def _(k):
            for e in range(2):
                c = 2 * k + e
                for s, value in enumerate(cut(part_of(3, cown, c))):
                    if i < 3:
                        acc[i, c * SPLIT + s] = value
                    else:
                        total[c, s] = value

    def close(c, offset):
        return dot_rows(near[c, offset], field[c, my_rows, :])

    def raise_total(c, value):
        for s, piece in enumerate(cut(value)):
            total[c, s] = total[c, s] + piece

    def raise_acc(c, value):
        for s, piece in enumerate(cut(value)):
            acc[2, c * SPLIT + s] = acc[2, c * SPLIT + s] + piece

    def near_field():
        @pl.loop(1, last)
        def _(c):
            raise_total(c, close(c, 1) + close(c - 1, 2) + close(c + 1, 0))

        raise_total(0, close(0, 1) + close(1, 0))
        raise_total(last, close(last, 1) + close(last - 1, 2))

    def halo_terms():
        for copy in halos:
            copy.wait_recv()
        raise_acc(y * last, close((1 - y) * last, (1 - y) * 2))
        raise_acc((1 - y) * last, dot_rows(hnear[...], hfield[...]))

    def turn(i, k):
        side = mix(k // pair, 1 - bits[i], bits[i])
        return side * pair + lax.rem(k, pair)

    def ready(i):
        v_copy(i).wait_recv()
        prepare(min(i, 2), vrecv.at[i])

    def partial_away(i):
        c_copy(i).wait_recv()

        @pl.loop(0, quad // 2)
        def _(k):
            for e in range(2):
                n = turn(i, 2 * k + e)
                c = theirs + n
                value = part_of(min(i, 2), crecv.at[i], c)
                if i < 3:
                    for s, piece in enumerate(cut(value)):
                        ksend[i, n, s] = (acc[i, c * SPLIT + s] + piece).astype(BF16)
                    k_copy(i, n).start()
                else:
                    raise_total(c, value)
                    q_copy(n).start()

    def partial_keep(i, first, count):
        @pl.loop(0, count // 2)
        def _(k):
            for e in range(2):
                c = mine + turn(i, first + 2 * k + e)
                value = part_of(min(i, 2), crecv.at[i], c)
                if i < 3:
                    for s, piece in enumerate(cut(value)):
                        acc[i, c * SPLIT + s] = acc[i, c * SPLIT + s] + piece
                else:
                    raise_total(c, value)

    def summed(i, n, s):
        return acc[i, (mine + n) * SPLIT + s] + krecv[i, n, s].astype(F32)

    def give_g(i):
        partial_keep(i, 0, pair)

        @pl.loop(0, pair)
        def _(m):
            n = (1 - bits[i]) * pair + m
            k_copy(i, n).wait_recv()
            for s in range(SPLIT):
                gsend[i, m * SPLIT + s] = summed(i, n, s).astype(BF16)
                g_copy(i, m * SPLIT + s).start()

    def give_y():
        @pl.loop(0, quad)
        def _(k):
            n = turn(2, k)
            k_copy(2, n).wait_recv()
            for s in range(SPLIT):
                ysend[n, s] = summed(2, n, s).astype(BF16)
            y_copy(n).start()

    def take_k(i):
        @pl.loop(0, pair)
        def _(m):
            k_copy(i, bits[i] * pair + m).wait_recv()

    def reduced(t, m, s):
        return acc[t, (mine + mix(t, x, y) * pair + m) * SPLIT + s]

    def pass_z(m):
        for s in range(SPLIT):
            for i in range(2):
                g_copy(i, m * SPLIT + s).wait_recv()
                n = bits[i] * pair + m
                value = summed(i, n, s) + grecv[i, m * SPLIT + s].astype(F32)
                acc[i, (mine + n) * SPLIT + s] = value
            zsend[m * SPLIT + s] = reduced(1 - u, m, s).astype(BF16)
            z_copy(m * SPLIT + s).start()

    def pass_x(m):
        for s in range(SPLIT):
            z_copy(m * SPLIT + s).wait_recv()
            value = reduced(u, m, s) + zrecv[m * SPLIT + s].astype(F32)
            xsend[m * SPLIT + s] = value.astype(BF16)
            x_copy(m * SPLIT + s).start()

    def gathered(n, s):
        return total[mine + n, s] + qrecv[n, s] + yrecv[n, s].astype(F32)

    def pass_f(m):
        n = (1 - x) * pair + m
        q_copy(n).wait_recv()
        y_copy(n).wait_recv()
        for s in range(SPLIT):
            fsend[m * SPLIT + s] = gathered(n, s).astype(BF16)
            f_copy(m * SPLIT + s).start()

    for i in (1, 0, 2):
        own(i)
    ready(1)
    ready(0)
    own(3)
    ready(2)
    partial_away(1)
    partial_away(0)
    give_g(1)
    give_g(0)
    halo_terms()
    partial_away(2)
    partial_keep(2, 0, quad)
    give_y()
    partial_keep(1, pair, pair)
    partial_keep(0, pair, pair)
    take_k(1)
    take_k(0)
    near_field()
    pass_z(0)
    ready(3)
    partial_away(3)
    for m in range(1, pair):
        pass_z(m)
    partial_keep(3, 0, quad)

    @pl.loop(0, pair)
    def _(m):
        pass_x(m)
        pass_f(m)

    @pl.loop(0, pair)
    def _(m):
        n = x * pair + m
        q_copy(n).wait_recv()
        y_copy(n).wait_recv()
        for s in range(SPLIT):
            piece = m * SPLIT + s
            f_copy(piece).wait_recv()
            value = gathered(n, s) + frecv[piece].astype(F32)
            x_copy(piece).wait_recv()
            out[(mine + n) * SPLIT + s] = (value + xrecv[piece].astype(F32)).astype(BF16)
            o_copy(piece).start()
            p_copy(n * SPLIT + s).start()

    @pl.loop(0, pair * SPLIT)
    def _(m):
        o_copy(m).wait_recv()
        p_copy((1 - x) * pair * SPLIT + m).start()

    @pl.loop(0, quad * SPLIT)
    def _(n):
        p_copy(n).wait_recv()
        p_copy(n).wait_send()

    for copy in halos:
        copy.wait_send()
    for i in range(4):
        v_copy(i).wait_send()
        c_copy(i).wait_send()

    @pl.loop(0, quad)
    def _(n):
        for i in range(3):
            k_copy(i, n).wait_send()
        q_copy(n).wait_send()
        y_copy(n).wait_send()

    @pl.loop(0, pair * SPLIT)
    def _(m):
        for i in range(2):
            g_copy(i, m).wait_send()
        z_copy(m).wait_send()
        x_copy(m).wait_send()
        f_copy(m).wait_send()
        o_copy(m).wait_send()


def slots_of(col_owner, owners, most):
    target = col_owner[:, 0]
    number = jnp.arange(target.shape[0], dtype=jnp.int32)
    same = (target[:, None] == target[None, :]) & (number[None, :] < number[:, None])
    slot = target * most + jnp.sum(same.astype(jnp.int32), axis=1)
    return slot[:, None] == jnp.arange(owners * most, dtype=jnp.int32)[None, :]


def table(held, clusters, facts):
    lift = [0] * (len(facts) - 1) + [clusters]
    tab = jnp.sum(jnp.where(held[None], jnp.stack(facts)[:, :, None], 0), axis=1)
    return tab + jnp.array(lift, jnp.int32)[:, None]


def shards(
    field_in,
    left_factors,
    right_factors,
    block_ranks,
    row_cluster,
    col_owner,
    col_cluster,
    near_blocks,
):
    owners, reps = lax.axis_size("rows"), lax.axis_size("rep")
    blocks, width, rank = left_factors.shape
    clusters, _, columns = field_in.shape
    share = near_blocks.shape[2]
    most = 5 * blocks // (4 * owners) + 1
    part = columns // PARTS
    depth = most * rank
    pad = -(-most // 16) * 16
    tall = depth + pad
    stages = reps.bit_length() - 1

    smem = pl.BlockSpec(memory_space=pltpu.SMEM)
    vmem = pl.BlockSpec(memory_space=pltpu.VMEM)
    dma = pltpu.SemaphoreType.DMA
    arrays = (
        field_in,
        jnp.swapaxes(left_factors, 1, 2),
        jnp.swapaxes(right_factors, 1, 2),
        near_blocks,
    )
    cubic = stages == 2 and owners == 2 ** 3 and (blocks - 1).bit_length() * most < 32
    cubic = cubic and columns <= width
    if cubic:
        quad, pair = clusters // 2, clusters // 4
        slab = (width // SPLIT, columns)
        keep = pltpu.VMEM
        gathered = pl.pallas_call(
            functools.partial(cube, most),
            out_shape=jax.ShapeDtypeStruct((clusters * SPLIT, *slab), BF16),
            in_specs=[smem] * 3 + [pl.BlockSpec(memory_space=pl.ANY)] * 4,
            out_specs=vmem,
            scratch_shapes=[
                *[keep(array.shape, BF16) for array in arrays],
                keep((blocks, rank, columns), BF16),
                keep((4, tall, width), BF16),
                keep((4, depth, columns), BF16),
                keep((4, tall, width), BF16),
                keep((4, depth, columns), BF16),
                keep((tall, width), BF16),
                keep((depth, columns), BF16),
                keep((4, width, depth), BF16),
                keep((4, depth, columns), BF16),
                keep((share, width), BF16),
                keep((share, columns), BF16),
                keep((clusters, SPLIT, *slab), F32),
                keep((3, clusters * SPLIT, *slab), F32),
                keep((3, quad, SPLIT, *slab), BF16),
                keep((3, quad, SPLIT, *slab), BF16),
                keep((quad, SPLIT, *slab), F32),
                keep((2, pair * SPLIT, *slab), BF16),
                keep((2, pair * SPLIT, *slab), BF16),
                keep((quad, SPLIT, *slab), BF16),
                keep((quad, SPLIT, *slab), BF16),
                *[keep((pair * SPLIT, *slab), BF16)] * 6,
                *[dma((4,))] * 7,
                *[dma((3, quad))] * 2,
                *[dma((quad,))] * 2,
                *[dma((2, pair * SPLIT))] * 2,
                *[dma((quad,))] * 2,
                *[dma((pair * SPLIT,))] * 6,
                *[dma(((pair + quad) * SPLIT,))] * 2,
            ],
            compiler_params=pltpu.CompilerParams(
                collective_id=0, has_side_effects=True, vmem_limit_bytes=60 * 1024 * 1024
            ),
        )(row_cluster, block_ranks, table(slots_of(col_owner, owners, most), clusters, [jnp.arange(blocks, dtype=jnp.int32), col_cluster - clusters]), *arrays)
        return gathered.reshape(field_in.shape).astype(F32)

    held = slots_of(col_owner, owners, most)
    number = jnp.arange(blocks, dtype=jnp.int32)
    halves = [clusters >> (t + 1) for t in range(stages)]
    steps = [
        pltpu.VMEM((PARTS, half, width, part), BF16 if t else F32) for t, half in enumerate(halves)
    ]
    gathered = pl.pallas_call(
        functools.partial(kernel, owners, reps, most),
        out_shape=jax.ShapeDtypeStruct(field_in.shape, BF16),
        in_specs=[smem] + [vmem] * 4,
        out_specs=vmem,
        scratch_shapes=[
            pltpu.VMEM((owners, depth, width), BF16),
            pltpu.VMEM((owners, depth, width), BF16),
            pltpu.VMEM((owners, width, depth), BF16),
            pltpu.VMEM((PARTS, owners, tall, part), BF16),
            pltpu.VMEM((PARTS, owners, tall, part), BF16),
            pltpu.VMEM((2, share, width), BF16),
            pltpu.VMEM((2, share, columns), BF16),
            pltpu.VMEM((PARTS, clusters, width, part), F32),
            *steps,
            *steps,
            dma((owners,)),
            dma((owners,)),
            dma((PARTS, owners)),
            dma((PARTS, owners)),
            dma((4,)),
            dma((4,)),
            *[dma((PARTS, stages))] * 4,
        ],
        compiler_params=pltpu.CompilerParams(
            collective_id=0, has_side_effects=True, vmem_limit_bytes=60 * 1024 * 1024
        ),
    )(table(held, clusters, [number, row_cluster, block_ranks, col_cluster - clusters]), *arrays)
    return gathered.astype(F32)


def solution(mesh):
    in_specs = (
        P("rows", None, None),
        P(("rows", "rep"), None, None),
        P(("rows", "rep"), None, None),
        P(("rows", "rep")),
        P(("rows", "rep")),
        P(("rows", "rep"), None),
        P(("rows", "rep")),
        P("rows", None, "rep", None),
    )
    out_specs = P("rows", None, None)
    return jax.shard_map(shards, mesh=mesh, in_specs=in_specs, out_specs=out_specs, check_vma=False)
```

```python
import functools

import jax
import jax.numpy as jnp
from jax import lax
from jax.experimental import pallas as pl
from jax.experimental.pallas import tpu as pltpu
from jax.sharding import PartitionSpec as P

MESH = pl.DeviceIdType.MESH
PARTS = 2
SPLIT = 2
SPOTS = (0, 0, 1, 1)
BF16 = jnp.bfloat16
F32 = jnp.float32


def dot_rows(left, right):
    return lax.dot_general(left, right, (((0,), (0,)), ((), ())), preferred_element_type=F32)


def kernel(
    owners, reps, most, tab, field, ut, vt, near, out,
    vsend, vrecv, vtr, csend, crecv, hnear, hfield, total, *rest,
):
    stages = reps.bit_length() - 1
    rsend, rrecv = rest[:stages], rest[stages:2 * stages]
    vs, vr, cs, cr, hs, hr, rs, rr, gs, gr = rest[2 * stages:]
    group = owners
    row, rep = lax.axis_index("rows"), lax.axis_index("rep")
    place_in = lax.rem(row, group)
    base = row - place_in
    blocks, rank, width = ut.shape
    clusters, _, columns = field.shape
    share = near.shape[2]
    part = columns // PARTS
    depth = most * rank
    peers = group - 1

    barrier = pltpu.get_barrier_semaphore()

    @pl.loop(1, owners)
    def _(d):
        pl.semaphore_signal(
            barrier, inc=1, device_id=(lax.rem(row + d, owners), rep), device_id_type=MESH
        )

    @pl.loop(1, reps)
    def _(d):
        pl.semaphore_signal(
            barrier, inc=1, device_id=(row, lax.rem(rep + d, reps)), device_id_type=MESH
        )

    def peer(d):
        return base + lax.rem(place_in + d, group)

    def turn(k):
        step = (k + 1) // 2
        return group // 2 + lax.rem(k, 2) * step - (1 - lax.rem(k, 2)) * step

    def v_copy(d):
        return pltpu.make_async_remote_copy(
            src_ref=vsend.at[d], dst_ref=vrecv.at[d], send_sem=vs.at[d], recv_sem=vr.at[d],
            device_id=(peer(d), rep), device_id_type=MESH,
        )

    def c_copy(h, d):
        return pltpu.make_async_remote_copy(
            src_ref=csend.at[h, d], dst_ref=crecv.at[h, d],
            send_sem=cs.at[h, d], recv_sem=cr.at[h, d],
            device_id=(peer(d), rep), device_id_type=MESH,
        )

    def pack(d, target, owner):
        for j in range(most):
            target[d, pl.ds(j * rank, rank), :] = vt[tab[0, owner * most + j]]

    def coeffs(d, target, owner):
        extra = csend.shape[2] - depth
        lines = lax.broadcasted_iota(jnp.int32, (extra, part), 0)
        marks = jnp.full((extra, part), clusters, jnp.int32)
        for j in range(most):
            slot = owner * most + j
            value = jnp.dot(ut[tab[0, slot]], field[tab[1, slot]], preferred_element_type=F32)
            kept = lax.broadcasted_iota(jnp.int32, (rank, columns), 0) < tab[2, slot]
            value = jnp.where(kept, value, 0.0).astype(BF16)
            for h in range(PARTS):
                target[h, d, pl.ds(j * rank, rank), :] = value[:, h * part:(h + 1) * part]
            marks = jnp.where(lines == j, tab[3, slot], marks)
        for h in range(PARTS):
            target[h, d, pl.ds(depth, extra), :] = marks.astype(F32).astype(BF16)

    my_rows = pl.ds(pl.multiple_of(rep * share, share), share)

    def halo_copies():
        made = []
        for side, cluster, offset, shift in ((0, clusters - 1, 2, 1), (1, 0, 0, owners - 1)):
            where = (lax.rem(row + shift, owners), rep)
            made.append(pltpu.make_async_remote_copy(
                src_ref=near.at[cluster, offset], dst_ref=hnear.at[side],
                send_sem=hs.at[2 * side], recv_sem=hr.at[2 * side],
                device_id=where, device_id_type=MESH,
            ))
            made.append(pltpu.make_async_remote_copy(
                src_ref=field.at[cluster, my_rows, :], dst_ref=hfield.at[side],
                send_sem=hs.at[2 * side + 1], recv_sem=hr.at[2 * side + 1],
                device_id=where, device_id_type=MESH,
            ))
        return made

    plan = []
    low, size = 0, clusters
    for t in range(stages):
        bit = lax.rem(rep // (1 << t), 2)
        half = size // 2
        partner = rep + (1 << t) * (1 - 2 * bit)
        plan.append((half, partner, low + bit * half, low + (1 - bit) * half))
        low, size = low + bit * half, half

    def labels_of(source, h, d):
        return jnp.concatenate(
            [
                jnp.broadcast_to(source[h, d, pl.ds(depth + j, 1), :].astype(F32), (rank, part))
                for j in range(most)
            ],
            axis=0,
        ).astype(BF16)

    def part_of(right, source, labels, h, d, c):
        label = jnp.asarray(c, jnp.int32).astype(F32).astype(BF16)
        picked = jnp.where(
            labels == label, source[h, d, pl.ds(0, depth), :], jnp.zeros((), BF16)
        )
        return jnp.dot(right[d], picked, preferred_element_type=F32)

    pl.semaphore_wait(barrier, owners + reps - 2)

    @pl.loop(0, peers)
    def _(k):
        d = turn(k)
        pack(d, vsend, peer(d))
        v_copy(d).start()

    halos = halo_copies()
    for copy in halos:
        copy.start()

    @pl.loop(0, peers)
    def _(k):
        d = turn(k)
        coeffs(d, csend, peer(d))
        c_copy(0, d).start()

    for h in range(1, PARTS):
        @pl.loop(0, peers)
        def _(k):
            c_copy(h, turn(k)).start()

    pack(0, vrecv, row)
    coeffs(0, crecv, row)

    def put(c, value):
        for h in range(PARTS):
            total[h, c] = value[:, h * part:(h + 1) * part]

    def add(c, value):
        for h in range(PARTS):
            total[h, c] = total[h, c] + value[:, h * part:(h + 1) * part]

    @pl.loop(0, clusters)
    def _(c):
        put(c, dot_rows(near[c, 1], field[c, my_rows, :]))

    @pl.loop(0, clusters - 1)
    def _(c):
        add(c + 1, dot_rows(near[c, 2], field[c, my_rows, :]))
        add(c, dot_rows(near[c + 1, 0], field[c + 1, my_rows, :]))

    for copy in halos:
        copy.wait_recv()
    add(0, dot_rows(hnear[0], hfield[0]))
    add(clusters - 1, dot_rows(hnear[1], hfield[1]))

    def far(h, d):
        if h == 0:
            vtr[d] = vrecv[d].T
        labels = labels_of(crecv, h, d)

        @pl.loop(0, clusters)
        def _(c):
            total[h, c] = total[h, c] + part_of(vtr, crecv, labels, h, d, c)

    def far_span(h, first, last):
        @pl.loop(first, last)
        def _(k):
            d = turn(peers - 1 - k)
            if h == 0:
                v_copy(d).wait_recv()
            c_copy(h, d).wait_recv()
            far(h, d)

    def r_copy(h, t):
        return pltpu.make_async_remote_copy(
            src_ref=rsend[t].at[h], dst_ref=rrecv[t].at[h],
            send_sem=rs.at[h, t], recv_sem=rr.at[h, t],
            device_id=(row, plan[t][1]), device_id_type=MESH,
        )

    def g_copy(h, t):
        half, partner, keep, _ = plan[t]
        block = out.at[pl.ds(keep, half), :, pl.ds(h * part, part)]
        return pltpu.make_async_remote_copy(
            src_ref=block, dst_ref=block, send_sem=gs.at[h, t], recv_sem=gr.at[h, t],
            device_id=(row, partner), device_id_type=MESH,
        )

    def give(h, t):
        half, _, _, away = plan[t]

        @pl.loop(0, half)
        def _(i):
            rsend[t][h, i] = total[h, away + i].astype(rsend[t].dtype)

        r_copy(h, t).start()

    def take(h, t):
        half, _, keep, _ = plan[t]
        r_copy(h, t).wait_recv()

        @pl.loop(0, half)
        def _(i):
            value = total[h, keep + i] + rrecv[t][h, i].astype(F32)
            if t == stages - 1:
                out[keep + i, :, pl.ds(h * part, part)] = value.astype(BF16)
            else:
                total[h, keep + i] = value

    def sequence(h):
        steps = [lambda: give(h, 0)]
        for t in range(stages):
            if t < stages - 1:
                steps.append(lambda t=t: (take(h, t), give(h, t + 1)))
            else:
                steps.append(lambda t=t: (take(h, t), g_copy(h, t).start()))
        for t in range(stages - 1, 0, -1):
            steps.append(lambda t=t: (g_copy(h, t).wait_recv(), g_copy(h, t - 1).start()))
        steps.append(lambda: g_copy(h, 0).wait_recv())
        return steps

    ahead, behind = sequence(0), sequence(1)
    far(0, 0)
    far_span(0, 0, peers)
    ahead[0]()
    for step in ahead[1:stages]:
        step()
    middle = peers // 2
    far(1, 0)
    far_span(1, 0, middle)
    ahead[stages]()
    far_span(1, middle, peers)
    behind[0]()
    later = ahead[stages + 1:]
    for place, step in enumerate(behind[1:]):
        if place < len(later):
            later[place]()
        step()

    @pl.loop(1, group)
    def _(d):
        v_copy(d).wait_send()
        for h in range(PARTS):
            c_copy(h, d).wait_send()

    for copy in halos:
        copy.wait_send()
    for h in range(PARTS):
        for t in range(stages):
            r_copy(h, t).wait_send()
            g_copy(h, t).wait_send()


def cube(
    most, rowc, ranks, owner_of, colc, field_hbm, ut_hbm, vt_hbm, near_hbm, out,
    field, ut, vt, near,
    cnat, vsend, csend, vrecv, crecv, vown, cown, vtr, labels, hnear, hfield, total, acc,
    ksend, krecv, qrecv, gsend, grecv, ysend, yrecv, zsend, zrecv,
    xsend, xrecv, fsend, frecv,
    ins, vs, vr, cs, cr, hs, hr, ks, kr, qs, qr, gs, gr, ys, yr, zs, zr, xs, xr, fs, fr, os, orr,
):
    owners, reps = lax.axis_size("rows"), lax.axis_size("rep")
    row, rep = lax.axis_index("rows"), lax.axis_index("rep")
    half = owners // 2
    w, u, y = row // half, lax.rem(row // 2, 2), lax.rem(row, 2)
    x, core = rep // 2, lax.rem(rep, 2)
    blocks, rank, width = ut.shape
    clusters, _, columns = field.shape
    share = near.shape[2]
    depth = most * rank
    pad = vsend.shape[1] - depth
    quad = clusters // 2
    pair = clusters // 4
    sub = width // SPLIT
    bits_of = (blocks - 1).bit_length()

    def at(w_, u_, y_):
        return w_ * half + u_ * 2 + y_

    def mix(t, one, two):
        return one * (1 - t) + two * t

    to_y = (at(w, u, 1 - y), rep)
    to_z = (at(w, 1 - u, y), rep)
    to_x = (row, (1 - x) * 2 + core)
    to_core = (row, x * 2 + 1 - core)
    to_across = (at(1 - w, u, y), rep)
    to_next = (lax.rem(row + mix(y, owners - 2, 2), owners), rep)
    to_prior = (lax.rem(row + mix(y, 2, owners - 2), owners), rep)
    partners = (to_y, to_z, to_x, to_core, to_across, to_next, to_prior)

    barrier = pltpu.get_barrier_semaphore()
    for where in partners:
        pl.semaphore_signal(barrier, inc=1, device_id=where, device_id_type=MESH)

    loads = [
        pltpu.make_async_copy(src, dst, ins.at[i])
        for i, (src, dst) in enumerate(
            ((vt_hbm, vt), (ut_hbm, ut), (field_hbm, field), (near_hbm, near))
        )
    ]
    for load in loads:
        load.start()

    sends = (
        (to_y, at(1 - w, 1 - u, 1 - y)),
        (to_y, at(1 - w, u, 1 - y)),
        (to_z, at(w, 1 - u, 1 - y)),
        (to_z, at(w, 1 - u, y)),
    )
    owns = (at(1 - w, 1 - u, y), at(1 - w, u, y), at(w, u, 1 - y), row)
    mine = core * quad
    theirs = (1 - core) * quad

    def remote(src, dst, send, recv, where):
        return pltpu.make_async_remote_copy(
            src_ref=src, dst_ref=dst, send_sem=send, recv_sem=recv,
            device_id=where, device_id_type=MESH,
        )

    def v_copy(i):
        return remote(vsend.at[i], vrecv.at[i], vs.at[i], vr.at[i], sends[i][0])

    def c_copy(i):
        return remote(csend.at[i], crecv.at[i], cs.at[i], cr.at[i], sends[i][0])

    def k_copy(i, n):
        return remote(ksend.at[i, n], krecv.at[i, n], ks.at[i, n], kr.at[i, n], to_core)

    def q_copy(n):
        return remote(total.at[theirs + n], qrecv.at[n], qs.at[n], qr.at[n], to_core)

    def g_copy(i, m):
        return remote(gsend.at[i, m], grecv.at[i, m], gs.at[i, m], gr.at[i, m], to_x)

    def y_copy(n):
        return remote(ysend.at[n], yrecv.at[n], ys.at[n], yr.at[n], to_y)

    def z_copy(m):
        return remote(zsend.at[m], zrecv.at[m], zs.at[m], zr.at[m], to_z)

    def x_copy(m):
        return remote(xsend.at[m], xrecv.at[m], xs.at[m], xr.at[m], to_across)

    def f_copy(m):
        return remote(fsend.at[m], frecv.at[m], fs.at[m], fr.at[m], to_x)

    def o_copy(m):
        block = out.at[(mine + x * pair) * SPLIT + m]
        return remote(block, block, os.at[m], orr.at[m], to_x)

    def p_copy(n):
        block = out.at[mine * SPLIT + n]
        spot = pair * SPLIT + n
        return remote(block, block, os.at[spot], orr.at[spot], to_core)

    def note(b, held):
        listed, counts = held[:owners], held[owners:]
        target = owner_of[b]
        hits = [target == o for o in range(owners)]
        return (
            *[jnp.where(hit, old * blocks + b, old) for hit, old in zip(hits, listed)],
            *[jnp.where(hit, old + 1, old) for hit, old in zip(hits, counts)],
        )

    noted = (jnp.int32(0),) * (2 * owners)
    for b in range(blocks):
        noted = note(b, noted)

    def slots_for(owner):
        listed, count = noted[0], noted[owners]
        for o in range(1, owners):
            listed = jnp.where(owner == o, noted[o], listed)
            count = jnp.where(owner == o, noted[owners + o], count)
        found = []
        for j in range(most):
            found.append((listed & (blocks - 1), j < count))
            listed = listed >> bits_of
        return found

    def pack_v(owner, put):
        lines = lax.broadcasted_iota(jnp.int32, (pad, width), 0)
        marks = jnp.full((pad, width), clusters, jnp.int32)
        for j, (block, valid) in enumerate(slots_for(owner)):
            put(pl.ds(j * rank, rank), vt[block])
            label = jnp.where(valid, colc[block], clusters)
            marks = jnp.where(lines == j, label, marks)
        put(pl.ds(depth, pad), marks.astype(F32).astype(BF16))

    def pack_c(owner, put):
        for j, (block, _) in enumerate(slots_for(owner)):
            put(pl.ds(j * rank, rank), cnat[block])

    def send_v(i):
        def put(spot, value):
            vsend[i, spot, :] = value

        pack_v(sends[i][1], put)

    def send_c(i):
        def put(spot, value):
            csend[i, spot, :] = value

        pack_c(sends[i][1], put)
        c_copy(i).start()

    my_rows = pl.ds(pl.multiple_of(rep * share, share), share)
    last = clusters - 1
    halos = [
        remote(near.at[y * last, y * 2], hnear, hs.at[0], hr.at[0], to_next),
        remote(field.at[y * last, my_rows, :], hfield, hs.at[1], hr.at[1], to_next),
    ]

    loads[0].wait()
    for i in range(4):
        send_v(i)
    for load in loads[1:]:
        load.wait()
    pl.semaphore_wait(barrier, len(partners))
    v_copy(0).start()
    for copy in halos:
        copy.start()
    v_copy(2).start()

    def coefficients(b):
        value = jnp.dot(ut[b], field[rowc[b]], preferred_element_type=F32)
        kept = lax.broadcasted_iota(jnp.int32, (rank, columns), 0) < ranks[b]
        cnat[b] = jnp.where(kept, value, 0.0).astype(BF16)

    @pl.loop(0, blocks // 4)
    def _(b):
        for e in range(4):
            coefficients(b * 4 + e)

    for i in (0, 2):
        send_c(i)
    for i in (1, 3):
        v_copy(i).start()
        send_c(i)

    def cut(value):
        return [value[s * sub:(s + 1) * sub] for s in range(SPLIT)]

    def prepare(d, factors):
        vtr[d] = factors[pl.ds(0, depth), :].T
        for j in range(most):
            line = factors[pl.ds(depth + j, 1), pl.ds(0, columns)].astype(F32)
            labels[d, pl.ds(j * rank, rank), :] = (
                jnp.broadcast_to(line, (rank, columns)).astype(BF16)
            )

    def part_of(d, coeffs, c):
        label = jnp.asarray(c, jnp.int32).astype(F32).astype(BF16)
        picked = jnp.where(labels[d] == label, coeffs[...], jnp.zeros((), BF16))
        return jnp.dot(vtr[d], picked, preferred_element_type=F32)

    def own(i):
        def put_v(spot, value):
            vown[spot, :] = value

        def put_c(spot, value):
            cown[spot, :] = value

        pack_v(owns[i], put_v)
        pack_c(owns[i], put_c)
        prepare(2, vown)

        @pl.loop(0, clusters // 2)
        def _(k):
            for e in range(2):
                c = 2 * k + e
                for s, value in enumerate(cut(part_of(2, cown, c))):
                    if i < 3:
                        acc[i, c * SPLIT + s] = value
                    else:
                        total[c, s] = value

    def close(c, offset):
        return dot_rows(near[c, offset], field[c, my_rows, :])

    def raise_total(c, value):
        for s, piece in enumerate(cut(value)):
            total[c, s] = total[c, s] + piece

    def raise_acc(c, value):
        for s, piece in enumerate(cut(value)):
            acc[2, c * SPLIT + s] = acc[2, c * SPLIT + s] + piece

    def near_field():
        @pl.loop(1, last)
        def _(c):
            raise_total(c, close(c, 1) + close(c - 1, 2) + close(c + 1, 0))

        raise_total(0, close(0, 1) + close(1, 0))
        raise_total(last, close(last, 1) + close(last - 1, 2))

    def halo_terms():
        for copy in halos:
            copy.wait_recv()
        raise_acc(y * last, close((1 - y) * last, (1 - y) * 2))
        raise_acc((1 - y) * last, dot_rows(hnear[...], hfield[...]))

    def turn(k):
        side = mix(k // pair, 1 - x, x)
        return side * pair + lax.rem(k, pair)

    def ready(i):
        v_copy(i).wait_recv()
        prepare(SPOTS[i], vrecv.at[i])

    def partial_away(i):
        c_copy(i).wait_recv()

        @pl.loop(0, quad // 2)
        def _(k):
            for e in range(2):
                n = turn(2 * k + e)
                c = theirs + n
                value = part_of(SPOTS[i], crecv.at[i], c)
                if i < 3:
                    for s, piece in enumerate(cut(value)):
                        ksend[i, n, s] = (acc[i, c * SPLIT + s] + piece).astype(BF16)
                    k_copy(i, n).start()
                else:
                    raise_total(c, value)
                    q_copy(n).start()

    def partial_keep(i, first, count):
        @pl.loop(0, count // 2)
        def _(k):
            for e in range(2):
                c = mine + turn(first + 2 * k + e)
                value = part_of(SPOTS[i], crecv.at[i], c)
                if i < 3:
                    for s, piece in enumerate(cut(value)):
                        acc[i, c * SPLIT + s] = acc[i, c * SPLIT + s] + piece
                else:
                    raise_total(c, value)

    def summed(i, n, s):
        return acc[i, (mine + n) * SPLIT + s] + krecv[i, n, s].astype(F32)

    def give_g(i):
        partial_keep(i, 0, pair)

        @pl.loop(0, pair)
        def _(m):
            n = (1 - x) * pair + m
            k_copy(i, n).wait_recv()
            for s in range(SPLIT):
                gsend[i, m * SPLIT + s] = summed(i, n, s).astype(BF16)
                g_copy(i, m * SPLIT + s).start()

    def give_y():
        @pl.loop(0, quad)
        def _(k):
            n = turn(k)
            k_copy(2, n).wait_recv()
            for s in range(SPLIT):
                ysend[n, s] = summed(2, n, s).astype(BF16)
            y_copy(n).start()

    def take_k(i):
        @pl.loop(0, pair)
        def _(m):
            k_copy(i, x * pair + m).wait_recv()

    def reduced(i, m, s):
        g_copy(i, m * SPLIT + s).wait_recv()
        return summed(i, x * pair + m, s) + grecv[i, m * SPLIT + s].astype(F32)

    def pass_z(m):
        for s in range(SPLIT):
            zsend[m * SPLIT + s] = reduced(0, m, s).astype(BF16)
            z_copy(m * SPLIT + s).start()

    def pass_x(m):
        for s in range(SPLIT):
            value = reduced(1, m, s)
            z_copy(m * SPLIT + s).wait_recv()
            xsend[m * SPLIT + s] = (value + zrecv[m * SPLIT + s].astype(F32)).astype(BF16)
            x_copy(m * SPLIT + s).start()

    def gathered(n, s):
        return total[mine + n, s] + qrecv[n, s] + yrecv[n, s].astype(F32)

    def pass_f(m):
        n = (1 - x) * pair + m
        q_copy(n).wait_recv()
        y_copy(n).wait_recv()
        for s in range(SPLIT):
            fsend[m * SPLIT + s] = gathered(n, s).astype(BF16)
            f_copy(m * SPLIT + s).start()

    for i in (0, 2):
        own(i)
    ready(0)
    own(1)
    own(3)
    ready(2)
    partial_away(0)
    give_g(0)
    halo_terms()
    partial_away(2)
    partial_keep(2, 0, quad)
    partial_keep(0, pair, pair)
    give_y()
    take_k(0)
    near_field()
    pass_z(0)
    ready(1)
    partial_away(1)
    give_g(1)
    for m in range(1, pair):
        pass_z(m)
    partial_keep(1, pair, pair)
    take_k(1)
    ready(3)
    partial_away(3)
    partial_keep(3, 0, quad)

    @pl.loop(0, pair)
    def _(m):
        pass_f(m)
        pass_x(m)

    @pl.loop(0, pair)
    def _(m):
        n = x * pair + m
        q_copy(n).wait_recv()
        y_copy(n).wait_recv()
        for s in range(SPLIT):
            piece = m * SPLIT + s
            f_copy(piece).wait_recv()
            value = gathered(n, s) + frecv[piece].astype(F32)
            x_copy(piece).wait_recv()
            out[(mine + n) * SPLIT + s] = (value + xrecv[piece].astype(F32)).astype(BF16)
            o_copy(piece).start()
            p_copy(n * SPLIT + s).start()

    @pl.loop(0, pair * SPLIT)
    def _(m):
        o_copy(m).wait_recv()
        p_copy((1 - x) * pair * SPLIT + m).start()

    @pl.loop(0, quad * SPLIT)
    def _(n):
        p_copy(n).wait_recv()
        p_copy(n).wait_send()

    for copy in halos:
        copy.wait_send()
    for i in range(4):
        v_copy(i).wait_send()
        c_copy(i).wait_send()

    @pl.loop(0, quad)
    def _(n):
        for i in range(3):
            k_copy(i, n).wait_send()
        q_copy(n).wait_send()
        y_copy(n).wait_send()

    @pl.loop(0, pair * SPLIT)
    def _(m):
        for i in range(2):
            g_copy(i, m).wait_send()
        z_copy(m).wait_send()
        x_copy(m).wait_send()
        f_copy(m).wait_send()
        o_copy(m).wait_send()


def slots_of(col_owner, owners, most):
    target = col_owner[:, 0]
    number = jnp.arange(target.shape[0], dtype=jnp.int32)
    same = (target[:, None] == target[None, :]) & (number[None, :] < number[:, None])
    slot = target * most + jnp.sum(same.astype(jnp.int32), axis=1)
    return slot[:, None] == jnp.arange(owners * most, dtype=jnp.int32)[None, :]


def table(held, clusters, facts):
    lift = [0] * (len(facts) - 1) + [clusters]
    tab = jnp.sum(jnp.where(held[None], jnp.stack(facts)[:, :, None], 0), axis=1)
    return tab + jnp.array(lift, jnp.int32)[:, None]


def shards(
    field_in,
    left_factors,
    right_factors,
    block_ranks,
    row_cluster,
    col_owner,
    col_cluster,
    near_blocks,
):
    owners, reps = lax.axis_size("rows"), lax.axis_size("rep")
    blocks, width, rank = left_factors.shape
    clusters, _, columns = field_in.shape
    share = near_blocks.shape[2]
    most = 5 * blocks // (4 * owners) + 1
    part = columns // PARTS
    depth = most * rank
    pad = -(-most // 16) * 16
    tall = depth + pad
    stages = reps.bit_length() - 1

    smem = pl.BlockSpec(memory_space=pltpu.SMEM)
    vmem = pl.BlockSpec(memory_space=pltpu.VMEM)
    dma = pltpu.SemaphoreType.DMA
    arrays = (
        field_in,
        jnp.swapaxes(left_factors, 1, 2),
        jnp.swapaxes(right_factors, 1, 2),
        near_blocks,
    )
    cubic = stages == 2 and owners == 2 ** 3 and (blocks - 1).bit_length() * most < 32
    cubic = cubic and blocks == 2 ** (blocks - 1).bit_length()
    cubic = cubic and columns <= width
    if cubic:
        quad, pair = clusters // 2, clusters // 4
        slab = (width // SPLIT, columns)
        keep = pltpu.VMEM
        gathered = pl.pallas_call(
            functools.partial(cube, most),
            out_shape=jax.ShapeDtypeStruct((clusters * SPLIT, *slab), BF16),
            in_specs=[smem] * 4 + [pl.BlockSpec(memory_space=pl.ANY)] * 4,
            out_specs=vmem,
            scratch_shapes=[
                *[keep(array.shape, BF16) for array in arrays],
                keep((blocks, rank, columns), BF16),
                keep((4, tall, width), BF16),
                keep((4, depth, columns), BF16),
                keep((4, tall, width), BF16),
                keep((4, depth, columns), BF16),
                keep((tall, width), BF16),
                keep((depth, columns), BF16),
                keep((3, width, depth), BF16),
                keep((3, depth, columns), BF16),
                keep((share, width), BF16),
                keep((share, columns), BF16),
                keep((clusters, SPLIT, *slab), F32),
                keep((3, clusters * SPLIT, *slab), F32),
                keep((3, quad, SPLIT, *slab), BF16),
                keep((3, quad, SPLIT, *slab), BF16),
                keep((quad, SPLIT, *slab), F32),
                keep((2, pair * SPLIT, *slab), BF16),
                keep((2, pair * SPLIT, *slab), BF16),
                keep((quad, SPLIT, *slab), BF16),
                keep((quad, SPLIT, *slab), BF16),
                *[keep((pair * SPLIT, *slab), BF16)] * 6,
                *[dma((4,))] * 7,
                *[dma((3, quad))] * 2,
                *[dma((quad,))] * 2,
                *[dma((2, pair * SPLIT))] * 2,
                *[dma((quad,))] * 2,
                *[dma((pair * SPLIT,))] * 6,
                *[dma(((pair + quad) * SPLIT,))] * 2,
            ],
            compiler_params=pltpu.CompilerParams(
                collective_id=0, has_side_effects=True, vmem_limit_bytes=60 * 1024 * 1024
            ),
        )(row_cluster, block_ranks, col_owner[:, 0], col_cluster, *arrays)
        return gathered.reshape(field_in.shape).astype(F32)

    held = slots_of(col_owner, owners, most)
    number = jnp.arange(blocks, dtype=jnp.int32)
    halves = [clusters >> (t + 1) for t in range(stages)]
    steps = [
        pltpu.VMEM((PARTS, half, width, part), BF16 if t else F32) for t, half in enumerate(halves)
    ]
    gathered = pl.pallas_call(
        functools.partial(kernel, owners, reps, most),
        out_shape=jax.ShapeDtypeStruct(field_in.shape, BF16),
        in_specs=[smem] + [vmem] * 4,
        out_specs=vmem,
        scratch_shapes=[
            pltpu.VMEM((owners, depth, width), BF16),
            pltpu.VMEM((owners, depth, width), BF16),
            pltpu.VMEM((owners, width, depth), BF16),
            pltpu.VMEM((PARTS, owners, tall, part), BF16),
            pltpu.VMEM((PARTS, owners, tall, part), BF16),
            pltpu.VMEM((2, share, width), BF16),
            pltpu.VMEM((2, share, columns), BF16),
            pltpu.VMEM((PARTS, clusters, width, part), F32),
            *steps,
            *steps,
            dma((owners,)),
            dma((owners,)),
            dma((PARTS, owners)),
            dma((PARTS, owners)),
            dma((4,)),
            dma((4,)),
            *[dma((PARTS, stages))] * 4,
        ],
        compiler_params=pltpu.CompilerParams(
            collective_id=0, has_side_effects=True, vmem_limit_bytes=60 * 1024 * 1024
        ),
    )(table(held, clusters, [number, row_cluster, block_ranks, col_cluster - clusters]), *arrays)
    return gathered.astype(F32)


def solution(mesh):
    in_specs = (
        P("rows", None, None),
        P(("rows", "rep"), None, None),
        P(("rows", "rep"), None, None),
        P(("rows", "rep")),
        P(("rows", "rep")),
        P(("rows", "rep"), None),
        P(("rows", "rep")),
        P("rows", None, "rep", None),
    )
    out_specs = P("rows", None, None)
    return jax.shard_map(shards, mesh=mesh, in_specs=in_specs, out_specs=out_specs, check_vma=False)
```

```python
import functools

import jax
import jax.numpy as jnp
from jax import lax
from jax.experimental import pallas as pl
from jax.experimental.pallas import tpu as pltpu
from jax.sharding import PartitionSpec as P

MESH = pl.DeviceIdType.MESH
PARTS = 2
SPLIT = 2
SPOTS = (0, 0, 1, 1)
BF16 = jnp.bfloat16
F32 = jnp.float32


def dot_rows(left, right):
    return lax.dot_general(left, right, (((0,), (0,)), ((), ())), preferred_element_type=F32)


def kernel(
    owners, reps, most, tab, field, ut, vt, near, out,
    vsend, vrecv, vtr, csend, crecv, hnear, hfield, total, *rest,
):
    stages = reps.bit_length() - 1
    rsend, rrecv = rest[:stages], rest[stages:2 * stages]
    vs, vr, cs, cr, hs, hr, rs, rr, gs, gr = rest[2 * stages:]
    group = owners
    row, rep = lax.axis_index("rows"), lax.axis_index("rep")
    place_in = lax.rem(row, group)
    base = row - place_in
    blocks, rank, width = ut.shape
    clusters, _, columns = field.shape
    share = near.shape[2]
    part = columns // PARTS
    depth = most * rank
    peers = group - 1

    barrier = pltpu.get_barrier_semaphore()

    @pl.loop(1, owners)
    def _(d):
        pl.semaphore_signal(
            barrier, inc=1, device_id=(lax.rem(row + d, owners), rep), device_id_type=MESH
        )

    @pl.loop(1, reps)
    def _(d):
        pl.semaphore_signal(
            barrier, inc=1, device_id=(row, lax.rem(rep + d, reps)), device_id_type=MESH
        )

    def peer(d):
        return base + lax.rem(place_in + d, group)

    def turn(k):
        step = (k + 1) // 2
        return group // 2 + lax.rem(k, 2) * step - (1 - lax.rem(k, 2)) * step

    def v_copy(d):
        return pltpu.make_async_remote_copy(
            src_ref=vsend.at[d], dst_ref=vrecv.at[d], send_sem=vs.at[d], recv_sem=vr.at[d],
            device_id=(peer(d), rep), device_id_type=MESH,
        )

    def c_copy(h, d):
        return pltpu.make_async_remote_copy(
            src_ref=csend.at[h, d], dst_ref=crecv.at[h, d],
            send_sem=cs.at[h, d], recv_sem=cr.at[h, d],
            device_id=(peer(d), rep), device_id_type=MESH,
        )

    def pack(d, target, owner):
        for j in range(most):
            target[d, pl.ds(j * rank, rank), :] = vt[tab[0, owner * most + j]]

    def coeffs(d, target, owner):
        extra = csend.shape[2] - depth
        lines = lax.broadcasted_iota(jnp.int32, (extra, part), 0)
        marks = jnp.full((extra, part), clusters, jnp.int32)
        for j in range(most):
            slot = owner * most + j
            value = jnp.dot(ut[tab[0, slot]], field[tab[1, slot]], preferred_element_type=F32)
            kept = lax.broadcasted_iota(jnp.int32, (rank, columns), 0) < tab[2, slot]
            value = jnp.where(kept, value, 0.0).astype(BF16)
            for h in range(PARTS):
                target[h, d, pl.ds(j * rank, rank), :] = value[:, h * part:(h + 1) * part]
            marks = jnp.where(lines == j, tab[3, slot], marks)
        for h in range(PARTS):
            target[h, d, pl.ds(depth, extra), :] = marks.astype(F32).astype(BF16)

    my_rows = pl.ds(pl.multiple_of(rep * share, share), share)

    def halo_copies():
        made = []
        for side, cluster, offset, shift in ((0, clusters - 1, 2, 1), (1, 0, 0, owners - 1)):
            where = (lax.rem(row + shift, owners), rep)
            made.append(pltpu.make_async_remote_copy(
                src_ref=near.at[cluster, offset], dst_ref=hnear.at[side],
                send_sem=hs.at[2 * side], recv_sem=hr.at[2 * side],
                device_id=where, device_id_type=MESH,
            ))
            made.append(pltpu.make_async_remote_copy(
                src_ref=field.at[cluster, my_rows, :], dst_ref=hfield.at[side],
                send_sem=hs.at[2 * side + 1], recv_sem=hr.at[2 * side + 1],
                device_id=where, device_id_type=MESH,
            ))
        return made

    plan = []
    low, size = 0, clusters
    for t in range(stages):
        bit = lax.rem(rep // (1 << t), 2)
        half = size // 2
        partner = rep + (1 << t) * (1 - 2 * bit)
        plan.append((half, partner, low + bit * half, low + (1 - bit) * half))
        low, size = low + bit * half, half

    def labels_of(source, h, d):
        return jnp.concatenate(
            [
                jnp.broadcast_to(source[h, d, pl.ds(depth + j, 1), :].astype(F32), (rank, part))
                for j in range(most)
            ],
            axis=0,
        ).astype(BF16)

    def part_of(right, source, labels, h, d, c):
        label = jnp.asarray(c, jnp.int32).astype(F32).astype(BF16)
        picked = jnp.where(
            labels == label, source[h, d, pl.ds(0, depth), :], jnp.zeros((), BF16)
        )
        return jnp.dot(right[d], picked, preferred_element_type=F32)

    pl.semaphore_wait(barrier, owners + reps - 2)

    @pl.loop(0, peers)
    def _(k):
        d = turn(k)
        pack(d, vsend, peer(d))
        v_copy(d).start()

    halos = halo_copies()
    for copy in halos:
        copy.start()

    @pl.loop(0, peers)
    def _(k):
        d = turn(k)
        coeffs(d, csend, peer(d))
        c_copy(0, d).start()

    for h in range(1, PARTS):
        @pl.loop(0, peers)
        def _(k):
            c_copy(h, turn(k)).start()

    pack(0, vrecv, row)
    coeffs(0, crecv, row)

    def put(c, value):
        for h in range(PARTS):
            total[h, c] = value[:, h * part:(h + 1) * part]

    def add(c, value):
        for h in range(PARTS):
            total[h, c] = total[h, c] + value[:, h * part:(h + 1) * part]

    @pl.loop(0, clusters)
    def _(c):
        put(c, dot_rows(near[c, 1], field[c, my_rows, :]))

    @pl.loop(0, clusters - 1)
    def _(c):
        add(c + 1, dot_rows(near[c, 2], field[c, my_rows, :]))
        add(c, dot_rows(near[c + 1, 0], field[c + 1, my_rows, :]))

    for copy in halos:
        copy.wait_recv()
    add(0, dot_rows(hnear[0], hfield[0]))
    add(clusters - 1, dot_rows(hnear[1], hfield[1]))

    def far(h, d):
        if h == 0:
            vtr[d] = vrecv[d].T
        labels = labels_of(crecv, h, d)

        @pl.loop(0, clusters)
        def _(c):
            total[h, c] = total[h, c] + part_of(vtr, crecv, labels, h, d, c)

    def far_span(h, first, last):
        @pl.loop(first, last)
        def _(k):
            d = turn(peers - 1 - k)
            if h == 0:
                v_copy(d).wait_recv()
            c_copy(h, d).wait_recv()
            far(h, d)

    def r_copy(h, t):
        return pltpu.make_async_remote_copy(
            src_ref=rsend[t].at[h], dst_ref=rrecv[t].at[h],
            send_sem=rs.at[h, t], recv_sem=rr.at[h, t],
            device_id=(row, plan[t][1]), device_id_type=MESH,
        )

    def g_copy(h, t):
        half, partner, keep, _ = plan[t]
        block = out.at[pl.ds(keep, half), :, pl.ds(h * part, part)]
        return pltpu.make_async_remote_copy(
            src_ref=block, dst_ref=block, send_sem=gs.at[h, t], recv_sem=gr.at[h, t],
            device_id=(row, partner), device_id_type=MESH,
        )

    def give(h, t):
        half, _, _, away = plan[t]

        @pl.loop(0, half)
        def _(i):
            rsend[t][h, i] = total[h, away + i].astype(rsend[t].dtype)

        r_copy(h, t).start()

    def take(h, t):
        half, _, keep, _ = plan[t]
        r_copy(h, t).wait_recv()

        @pl.loop(0, half)
        def _(i):
            value = total[h, keep + i] + rrecv[t][h, i].astype(F32)
            if t == stages - 1:
                out[keep + i, :, pl.ds(h * part, part)] = value.astype(BF16)
            else:
                total[h, keep + i] = value

    def sequence(h):
        steps = [lambda: give(h, 0)]
        for t in range(stages):
            if t < stages - 1:
                steps.append(lambda t=t: (take(h, t), give(h, t + 1)))
            else:
                steps.append(lambda t=t: (take(h, t), g_copy(h, t).start()))
        for t in range(stages - 1, 0, -1):
            steps.append(lambda t=t: (g_copy(h, t).wait_recv(), g_copy(h, t - 1).start()))
        steps.append(lambda: g_copy(h, 0).wait_recv())
        return steps

    ahead, behind = sequence(0), sequence(1)
    far(0, 0)
    far_span(0, 0, peers)
    ahead[0]()
    for step in ahead[1:stages]:
        step()
    middle = peers // 2
    far(1, 0)
    far_span(1, 0, middle)
    ahead[stages]()
    far_span(1, middle, peers)
    behind[0]()
    later = ahead[stages + 1:]
    for place, step in enumerate(behind[1:]):
        if place < len(later):
            later[place]()
        step()

    @pl.loop(1, group)
    def _(d):
        v_copy(d).wait_send()
        for h in range(PARTS):
            c_copy(h, d).wait_send()

    for copy in halos:
        copy.wait_send()
    for h in range(PARTS):
        for t in range(stages):
            r_copy(h, t).wait_send()
            g_copy(h, t).wait_send()


def cube(
    most, facts_hbm, field_hbm, ut_hbm, vt_hbm, near_hbm, out,
    facts, field, ut, vt, near,
    cnat, vsend, csend, vrecv, crecv, vown, cown, vtr, labels, hnear, hfield, total, acc,
    ksend, krecv, qrecv, gsend, grecv, ysend, yrecv, zsend, zrecv,
    xsend, xrecv, fsend, frecv,
    ins, vs, vr, cs, cr, hs, hr, ks, kr, qs, qr, gs, gr, ys, yr, zs, zr, xs, xr, fs, fr, os, orr,
):
    owners, reps = lax.axis_size("rows"), lax.axis_size("rep")
    row, rep = lax.axis_index("rows"), lax.axis_index("rep")
    half = owners // 2
    w, u, y = row // half, lax.rem(row // 2, 2), lax.rem(row, 2)
    x, core = rep // 2, lax.rem(rep, 2)
    blocks, rank, width = ut.shape
    clusters, _, columns = field.shape
    share = near.shape[2]
    depth = most * rank
    pad = vsend.shape[1] - depth
    quad = clusters // 2
    pair = clusters // 4
    sub = width // SPLIT
    bits_of = (blocks - 1).bit_length()

    def at(w_, u_, y_):
        return w_ * half + u_ * 2 + y_

    def mix(t, one, two):
        return one * (1 - t) + two * t

    to_y = (at(w, u, 1 - y), rep)
    to_z = (at(w, 1 - u, y), rep)
    to_x = (row, (1 - x) * 2 + core)
    to_core = (row, x * 2 + 1 - core)
    to_across = (at(1 - w, u, y), rep)
    to_next = (lax.rem(row + mix(y, owners - 2, 2), owners), rep)
    to_prior = (lax.rem(row + mix(y, 2, owners - 2), owners), rep)
    partners = (to_y, to_z, to_x, to_core, to_across, to_next, to_prior)

    barrier = pltpu.get_barrier_semaphore()
    for where in partners:
        pl.semaphore_signal(barrier, inc=1, device_id=where, device_id_type=MESH)

    loads = [
        pltpu.make_async_copy(src, dst, ins.at[i])
        for i, (src, dst) in enumerate(
            (
                (facts_hbm, facts), (vt_hbm, vt), (ut_hbm, ut),
                (field_hbm, field), (near_hbm, near),
            )
        )
    ]
    for load in loads:
        load.start()

    sends = (
        (to_y, at(1 - w, 1 - u, 1 - y)),
        (to_y, at(1 - w, u, 1 - y)),
        (to_z, at(w, 1 - u, 1 - y)),
        (to_z, at(w, 1 - u, y)),
    )
    owns = (at(1 - w, 1 - u, y), at(1 - w, u, y), at(w, u, 1 - y), row)
    mine = core * quad
    theirs = (1 - core) * quad

    def remote(src, dst, send, recv, where):
        return pltpu.make_async_remote_copy(
            src_ref=src, dst_ref=dst, send_sem=send, recv_sem=recv,
            device_id=where, device_id_type=MESH,
        )

    def v_copy(i):
        return remote(vsend.at[i], vrecv.at[i], vs.at[i], vr.at[i], sends[i][0])

    def c_copy(i):
        return remote(csend.at[i], crecv.at[i], cs.at[i], cr.at[i], sends[i][0])

    def k_copy(i, n):
        return remote(ksend.at[i, n], krecv.at[i, n], ks.at[i, n], kr.at[i, n], to_core)

    def q_copy(n):
        return remote(total.at[theirs + n], qrecv.at[n], qs.at[n], qr.at[n], to_core)

    def g_copy(i, m):
        return remote(gsend.at[i, m], grecv.at[i, m], gs.at[i, m], gr.at[i, m], to_x)

    def y_copy(n):
        return remote(ysend.at[n], yrecv.at[n], ys.at[n], yr.at[n], to_y)

    def z_copy(m):
        return remote(zsend.at[m], zrecv.at[m], zs.at[m], zr.at[m], to_z)

    def x_copy(m):
        return remote(xsend.at[m], xrecv.at[m], xs.at[m], xr.at[m], to_across)

    def f_copy(m):
        return remote(fsend.at[m], frecv.at[m], fs.at[m], fr.at[m], to_x)

    def o_copy(m):
        block = out.at[(mine + x * pair) * SPLIT + m]
        return remote(block, block, os.at[m], orr.at[m], to_x)

    def p_copy(n):
        block = out.at[mine * SPLIT + n]
        spot = pair * SPLIT + n
        return remote(block, block, os.at[spot], orr.at[spot], to_core)

    def note(b, held):
        listed, counts = held[:owners], held[owners:]
        target = facts[0, b]
        hits = [target == o for o in range(owners)]
        return (
            *[jnp.where(hit, old * blocks + b, old) for hit, old in zip(hits, listed)],
            *[jnp.where(hit, old + 1, old) for hit, old in zip(hits, counts)],
        )

    loads[0].wait()
    noted = (jnp.int32(0),) * (2 * owners)
    for b in range(blocks):
        noted = note(b, noted)

    def slots_for(owner):
        listed, count = noted[0], noted[owners]
        for o in range(1, owners):
            listed = jnp.where(owner == o, noted[o], listed)
            count = jnp.where(owner == o, noted[owners + o], count)
        found = []
        for j in range(most):
            found.append((listed & (blocks - 1), j < count))
            listed = listed >> bits_of
        return found

    def pack_v(owner, put):
        lines = lax.broadcasted_iota(jnp.int32, (pad, width), 0)
        marks = jnp.full((pad, width), clusters, jnp.int32)
        for j, (block, valid) in enumerate(slots_for(owner)):
            put(pl.ds(j * rank, rank), vt[block])
            label = jnp.where(valid, facts[1, block], clusters)
            marks = jnp.where(lines == j, label, marks)
        put(pl.ds(depth, pad), marks.astype(F32).astype(BF16))

    def pack_c(owner, put):
        for j, (block, _) in enumerate(slots_for(owner)):
            put(pl.ds(j * rank, rank), cnat[block])

    def send_v(i):
        def put(spot, value):
            vsend[i, spot, :] = value

        pack_v(sends[i][1], put)

    def send_c(i):
        def put(spot, value):
            csend[i, spot, :] = value

        pack_c(sends[i][1], put)
        c_copy(i).start()

    my_rows = pl.ds(pl.multiple_of(rep * share, share), share)
    last = clusters - 1
    halos = [
        remote(near.at[y * last, y * 2], hnear, hs.at[0], hr.at[0], to_next),
        remote(field.at[y * last, my_rows, :], hfield, hs.at[1], hr.at[1], to_next),
    ]

    loads[1].wait()
    for i in range(4):
        send_v(i)
    for load in loads[2:]:
        load.wait()
    pl.semaphore_wait(barrier, len(partners))
    v_copy(0).start()
    for copy in halos:
        copy.start()
    v_copy(2).start()

    def coefficients(b):
        value = jnp.dot(ut[b], field[facts[2, b]], preferred_element_type=F32)
        kept = lax.broadcasted_iota(jnp.int32, (rank, columns), 0) < facts[3, b]
        cnat[b] = jnp.where(kept, value, 0.0).astype(BF16)

    @pl.loop(0, blocks // 4)
    def _(b):
        for e in range(4):
            coefficients(b * 4 + e)

    for i in (0, 2):
        send_c(i)
    for i in (1, 3):
        v_copy(i).start()
        send_c(i)

    def cut(value):
        return [value[s * sub:(s + 1) * sub] for s in range(SPLIT)]

    def prepare(d, factors):
        vtr[d] = factors[pl.ds(0, depth), :].T
        for j in range(most):
            line = factors[pl.ds(depth + j, 1), pl.ds(0, columns)].astype(F32)
            labels[d, pl.ds(j * rank, rank), :] = (
                jnp.broadcast_to(line, (rank, columns)).astype(BF16)
            )

    def part_of(d, coeffs, c):
        label = jnp.asarray(c, jnp.int32).astype(F32).astype(BF16)
        picked = jnp.where(labels[d] == label, coeffs[...], jnp.zeros((), BF16))
        return jnp.dot(vtr[d], picked, preferred_element_type=F32)

    def own(i):
        def put_v(spot, value):
            vown[spot, :] = value

        def put_c(spot, value):
            cown[spot, :] = value

        pack_v(owns[i], put_v)
        pack_c(owns[i], put_c)
        prepare(2, vown)

        @pl.loop(0, clusters // 2)
        def _(k):
            for e in range(2):
                c = 2 * k + e
                for s, value in enumerate(cut(part_of(2, cown, c))):
                    if i < 3:
                        acc[i, c * SPLIT + s] = value
                    else:
                        total[c, s] = value

    def close(c, offset):
        return dot_rows(near[c, offset], field[c, my_rows, :])

    def raise_total(c, value):
        for s, piece in enumerate(cut(value)):
            total[c, s] = total[c, s] + piece

    def raise_acc(c, value):
        for s, piece in enumerate(cut(value)):
            acc[2, c * SPLIT + s] = acc[2, c * SPLIT + s] + piece

    def near_field():
        @pl.loop(1, last)
        def _(c):
            raise_total(c, close(c, 1) + close(c - 1, 2) + close(c + 1, 0))

        raise_total(0, close(0, 1) + close(1, 0))
        raise_total(last, close(last, 1) + close(last - 1, 2))

    def halo_terms():
        for copy in halos:
            copy.wait_recv()
        raise_acc(y * last, close((1 - y) * last, (1 - y) * 2))
        raise_acc((1 - y) * last, dot_rows(hnear[...], hfield[...]))

    def turn(k):
        side = mix(k // pair, 1 - x, x)
        return side * pair + lax.rem(k, pair)

    def ready(i):
        v_copy(i).wait_recv()
        prepare(SPOTS[i], vrecv.at[i])

    def partial_away(i):
        c_copy(i).wait_recv()

        @pl.loop(0, quad // 2)
        def _(k):
            for e in range(2):
                n = turn(2 * k + e)
                c = theirs + n
                value = part_of(SPOTS[i], crecv.at[i], c)
                if i < 3:
                    for s, piece in enumerate(cut(value)):
                        ksend[i, n, s] = (acc[i, c * SPLIT + s] + piece).astype(BF16)
                    k_copy(i, n).start()
                else:
                    raise_total(c, value)
                    q_copy(n).start()

    def partial_keep(i, first, count):
        @pl.loop(0, count // 2)
        def _(k):
            for e in range(2):
                c = mine + turn(first + 2 * k + e)
                value = part_of(SPOTS[i], crecv.at[i], c)
                if i < 3:
                    for s, piece in enumerate(cut(value)):
                        acc[i, c * SPLIT + s] = acc[i, c * SPLIT + s] + piece
                else:
                    raise_total(c, value)

    def summed(i, n, s):
        return acc[i, (mine + n) * SPLIT + s] + krecv[i, n, s].astype(F32)

    def give_g(i):
        partial_keep(i, 0, pair)

        @pl.loop(0, pair)
        def _(m):
            n = (1 - x) * pair + m
            k_copy(i, n).wait_recv()
            for s in range(SPLIT):
                gsend[i, m * SPLIT + s] = summed(i, n, s).astype(BF16)
                g_copy(i, m * SPLIT + s).start()

    def give_y():
        @pl.loop(0, quad)
        def _(k):
            n = turn(k)
            k_copy(2, n).wait_recv()
            for s in range(SPLIT):
                ysend[n, s] = summed(2, n, s).astype(BF16)
            y_copy(n).start()

    def take_k(i):
        @pl.loop(0, pair)
        def _(m):
            k_copy(i, x * pair + m).wait_recv()

    def reduced(i, m, s):
        g_copy(i, m * SPLIT + s).wait_recv()
        return summed(i, x * pair + m, s) + grecv[i, m * SPLIT + s].astype(F32)

    def pass_z(m):
        for s in range(SPLIT):
            zsend[m * SPLIT + s] = reduced(0, m, s).astype(BF16)
            z_copy(m * SPLIT + s).start()

    def pass_x(m):
        for s in range(SPLIT):
            value = reduced(1, m, s)
            z_copy(m * SPLIT + s).wait_recv()
            xsend[m * SPLIT + s] = (value + zrecv[m * SPLIT + s].astype(F32)).astype(BF16)
            x_copy(m * SPLIT + s).start()

    def gathered(n, s):
        return total[mine + n, s] + qrecv[n, s] + yrecv[n, s].astype(F32)

    def pass_f(m):
        n = (1 - x) * pair + m
        q_copy(n).wait_recv()
        y_copy(n).wait_recv()
        for s in range(SPLIT):
            fsend[m * SPLIT + s] = gathered(n, s).astype(BF16)
            f_copy(m * SPLIT + s).start()

    for i in (0, 2):
        own(i)
    ready(0)
    own(1)
    own(3)
    ready(2)
    partial_away(0)
    give_g(0)
    halo_terms()
    partial_away(2)
    partial_keep(2, 0, quad)
    partial_keep(0, pair, pair)
    give_y()
    take_k(0)
    near_field()
    pass_z(0)
    ready(1)
    partial_away(1)
    give_g(1)
    for m in range(1, pair):
        pass_z(m)
    partial_keep(1, pair, pair)
    take_k(1)
    ready(3)
    partial_away(3)
    partial_keep(3, 0, quad)

    @pl.loop(0, pair)
    def _(m):
        pass_f(m)
        pass_x(m)

    @pl.loop(0, pair)
    def _(m):
        n = x * pair + m
        q_copy(n).wait_recv()
        y_copy(n).wait_recv()
        for s in range(SPLIT):
            piece = m * SPLIT + s
            f_copy(piece).wait_recv()
            value = gathered(n, s) + frecv[piece].astype(F32)
            x_copy(piece).wait_recv()
            out[(mine + n) * SPLIT + s] = (value + xrecv[piece].astype(F32)).astype(BF16)
            o_copy(piece).start()
            p_copy(n * SPLIT + s).start()

    @pl.loop(0, pair * SPLIT)
    def _(m):
        o_copy(m).wait_recv()
        p_copy((1 - x) * pair * SPLIT + m).start()

    @pl.loop(0, quad * SPLIT)
    def _(n):
        p_copy(n).wait_recv()
        p_copy(n).wait_send()

    for copy in halos:
        copy.wait_send()
    for i in range(4):
        v_copy(i).wait_send()
        c_copy(i).wait_send()

    @pl.loop(0, quad)
    def _(n):
        for i in range(3):
            k_copy(i, n).wait_send()
        q_copy(n).wait_send()
        y_copy(n).wait_send()

    @pl.loop(0, pair * SPLIT)
    def _(m):
        for i in range(2):
            g_copy(i, m).wait_send()
        z_copy(m).wait_send()
        x_copy(m).wait_send()
        f_copy(m).wait_send()
        o_copy(m).wait_send()


def slots_of(col_owner, owners, most):
    target = col_owner[:, 0]
    number = jnp.arange(target.shape[0], dtype=jnp.int32)
    same = (target[:, None] == target[None, :]) & (number[None, :] < number[:, None])
    slot = target * most + jnp.sum(same.astype(jnp.int32), axis=1)
    return slot[:, None] == jnp.arange(owners * most, dtype=jnp.int32)[None, :]


def table(held, clusters, facts):
    lift = [0] * (len(facts) - 1) + [clusters]
    tab = jnp.sum(jnp.where(held[None], jnp.stack(facts)[:, :, None], 0), axis=1)
    return tab + jnp.array(lift, jnp.int32)[:, None]


def shards(
    field_in,
    left_factors,
    right_factors,
    block_ranks,
    row_cluster,
    col_owner,
    col_cluster,
    near_blocks,
):
    owners, reps = lax.axis_size("rows"), lax.axis_size("rep")
    blocks, width, rank = left_factors.shape
    clusters, _, columns = field_in.shape
    share = near_blocks.shape[2]
    most = 5 * blocks // (4 * owners) + 1
    part = columns // PARTS
    depth = most * rank
    pad = -(-most // 16) * 16
    tall = depth + pad
    stages = reps.bit_length() - 1

    smem = pl.BlockSpec(memory_space=pltpu.SMEM)
    vmem = pl.BlockSpec(memory_space=pltpu.VMEM)
    dma = pltpu.SemaphoreType.DMA
    arrays = (
        field_in,
        jnp.swapaxes(left_factors, 1, 2),
        jnp.swapaxes(right_factors, 1, 2),
        near_blocks,
    )
    cubic = stages == 2 and owners == 2 ** 3 and (blocks - 1).bit_length() * most < 32
    cubic = cubic and blocks == 2 ** (blocks - 1).bit_length()
    cubic = cubic and columns <= width
    if cubic:
        quad, pair = clusters // 2, clusters // 4
        slab = (width // SPLIT, columns)
        keep = pltpu.VMEM
        gathered = pl.pallas_call(
            functools.partial(cube, most),
            out_shape=jax.ShapeDtypeStruct((clusters * SPLIT, *slab), BF16),
            in_specs=[pl.BlockSpec(memory_space=pltpu.HBM)] * 5,
            out_specs=vmem,
            scratch_shapes=[
                pltpu.SMEM((4, blocks), jnp.int32),
                *[keep(array.shape, BF16) for array in arrays],
                keep((blocks, rank, columns), BF16),
                keep((4, tall, width), BF16),
                keep((4, depth, columns), BF16),
                keep((4, tall, width), BF16),
                keep((4, depth, columns), BF16),
                keep((tall, width), BF16),
                keep((depth, columns), BF16),
                keep((3, width, depth), BF16),
                keep((3, depth, columns), BF16),
                keep((share, width), BF16),
                keep((share, columns), BF16),
                keep((clusters, SPLIT, *slab), F32),
                keep((3, clusters * SPLIT, *slab), F32),
                keep((3, quad, SPLIT, *slab), BF16),
                keep((3, quad, SPLIT, *slab), BF16),
                keep((quad, SPLIT, *slab), F32),
                keep((2, pair * SPLIT, *slab), BF16),
                keep((2, pair * SPLIT, *slab), BF16),
                keep((quad, SPLIT, *slab), BF16),
                keep((quad, SPLIT, *slab), BF16),
                *[keep((pair * SPLIT, *slab), BF16)] * 6,
                dma((5,)),
                *[dma((4,))] * 6,
                *[dma((3, quad))] * 2,
                *[dma((quad,))] * 2,
                *[dma((2, pair * SPLIT))] * 2,
                *[dma((quad,))] * 2,
                *[dma((pair * SPLIT,))] * 6,
                *[dma(((pair + quad) * SPLIT,))] * 2,
            ],
            compiler_params=pltpu.CompilerParams(
                collective_id=0, has_side_effects=True, vmem_limit_bytes=52 * 1024 * 1024
            ),
        )(jnp.stack([col_owner[:, 0], col_cluster, row_cluster, block_ranks]), *arrays)
        return gathered.reshape(field_in.shape).astype(F32)

    held = slots_of(col_owner, owners, most)
    number = jnp.arange(blocks, dtype=jnp.int32)
    halves = [clusters >> (t + 1) for t in range(stages)]
    steps = [
        pltpu.VMEM((PARTS, half, width, part), BF16 if t else F32) for t, half in enumerate(halves)
    ]
    gathered = pl.pallas_call(
        functools.partial(kernel, owners, reps, most),
        out_shape=jax.ShapeDtypeStruct(field_in.shape, BF16),
        in_specs=[smem] + [vmem] * 4,
        out_specs=vmem,
        scratch_shapes=[
            pltpu.VMEM((owners, depth, width), BF16),
            pltpu.VMEM((owners, depth, width), BF16),
            pltpu.VMEM((owners, width, depth), BF16),
            pltpu.VMEM((PARTS, owners, tall, part), BF16),
            pltpu.VMEM((PARTS, owners, tall, part), BF16),
            pltpu.VMEM((2, share, width), BF16),
            pltpu.VMEM((2, share, columns), BF16),
            pltpu.VMEM((PARTS, clusters, width, part), F32),
            *steps,
            *steps,
            dma((owners,)),
            dma((owners,)),
            dma((PARTS, owners)),
            dma((PARTS, owners)),
            dma((4,)),
            dma((4,)),
            *[dma((PARTS, stages))] * 4,
        ],
        compiler_params=pltpu.CompilerParams(
            collective_id=0, has_side_effects=True, vmem_limit_bytes=60 * 1024 * 1024
        ),
    )(table(held, clusters, [number, row_cluster, block_ranks, col_cluster - clusters]), *arrays)
    return gathered.astype(F32)


def solution(mesh):
    in_specs = (
        P("rows", None, None),
        P(("rows", "rep"), None, None),
        P(("rows", "rep"), None, None),
        P(("rows", "rep")),
        P(("rows", "rep")),
        P(("rows", "rep"), None),
        P(("rows", "rep")),
        P("rows", None, "rep", None),
    )
    out_specs = P("rows", None, None)
    return jax.shard_map(shards, mesh=mesh, in_specs=in_specs, out_specs=out_specs, check_vma=False)
```

```python
import functools

import jax
import jax.numpy as jnp
from jax import lax
from jax.experimental import pallas as pl
from jax.experimental.pallas import tpu as pltpu
from jax.sharding import PartitionSpec as P

MESH = pl.DeviceIdType.MESH
PARTS = 2
SPLIT = 2
SPOTS = (0, 0, 1, 1)
BF16 = jnp.bfloat16
F32 = jnp.float32


def dot_rows(left, right):
    return lax.dot_general(left, right, (((0,), (0,)), ((), ())), preferred_element_type=F32)


def kernel(
    owners, reps, most, tab, field, ut, vt, near, out,
    vsend, vrecv, vtr, csend, crecv, hnear, hfield, total, *rest,
):
    stages = reps.bit_length() - 1
    rsend, rrecv = rest[:stages], rest[stages:2 * stages]
    vs, vr, cs, cr, hs, hr, rs, rr, gs, gr = rest[2 * stages:]
    group = owners
    row, rep = lax.axis_index("rows"), lax.axis_index("rep")
    place_in = lax.rem(row, group)
    base = row - place_in
    blocks, rank, width = ut.shape
    clusters, _, columns = field.shape
    share = near.shape[2]
    part = columns // PARTS
    depth = most * rank
    peers = group - 1

    barrier = pltpu.get_barrier_semaphore()

    @pl.loop(1, owners)
    def _(d):
        pl.semaphore_signal(
            barrier, inc=1, device_id=(lax.rem(row + d, owners), rep), device_id_type=MESH
        )

    @pl.loop(1, reps)
    def _(d):
        pl.semaphore_signal(
            barrier, inc=1, device_id=(row, lax.rem(rep + d, reps)), device_id_type=MESH
        )

    def peer(d):
        return base + lax.rem(place_in + d, group)

    def turn(k):
        step = (k + 1) // 2
        return group // 2 + lax.rem(k, 2) * step - (1 - lax.rem(k, 2)) * step

    def v_copy(d):
        return pltpu.make_async_remote_copy(
            src_ref=vsend.at[d], dst_ref=vrecv.at[d], send_sem=vs.at[d], recv_sem=vr.at[d],
            device_id=(peer(d), rep), device_id_type=MESH,
        )

    def c_copy(h, d):
        return pltpu.make_async_remote_copy(
            src_ref=csend.at[h, d], dst_ref=crecv.at[h, d],
            send_sem=cs.at[h, d], recv_sem=cr.at[h, d],
            device_id=(peer(d), rep), device_id_type=MESH,
        )

    def pack(d, target, owner):
        for j in range(most):
            target[d, pl.ds(j * rank, rank), :] = vt[tab[0, owner * most + j]]

    def coeffs(d, target, owner):
        extra = csend.shape[2] - depth
        lines = lax.broadcasted_iota(jnp.int32, (extra, part), 0)
        marks = jnp.full((extra, part), clusters, jnp.int32)
        for j in range(most):
            slot = owner * most + j
            value = jnp.dot(ut[tab[0, slot]], field[tab[1, slot]], preferred_element_type=F32)
            kept = lax.broadcasted_iota(jnp.int32, (rank, columns), 0) < tab[2, slot]
            value = jnp.where(kept, value, 0.0).astype(BF16)
            for h in range(PARTS):
                target[h, d, pl.ds(j * rank, rank), :] = value[:, h * part:(h + 1) * part]
            marks = jnp.where(lines == j, tab[3, slot], marks)
        for h in range(PARTS):
            target[h, d, pl.ds(depth, extra), :] = marks.astype(F32).astype(BF16)

    my_rows = pl.ds(pl.multiple_of(rep * share, share), share)

    def halo_copies():
        made = []
        for side, cluster, offset, shift in ((0, clusters - 1, 2, 1), (1, 0, 0, owners - 1)):
            where = (lax.rem(row + shift, owners), rep)
            made.append(pltpu.make_async_remote_copy(
                src_ref=near.at[cluster, offset], dst_ref=hnear.at[side],
                send_sem=hs.at[2 * side], recv_sem=hr.at[2 * side],
                device_id=where, device_id_type=MESH,
            ))
            made.append(pltpu.make_async_remote_copy(
                src_ref=field.at[cluster, my_rows, :], dst_ref=hfield.at[side],
                send_sem=hs.at[2 * side + 1], recv_sem=hr.at[2 * side + 1],
                device_id=where, device_id_type=MESH,
            ))
        return made

    plan = []
    low, size = 0, clusters
    for t in range(stages):
        bit = lax.rem(rep // (1 << t), 2)
        half = size // 2
        partner = rep + (1 << t) * (1 - 2 * bit)
        plan.append((half, partner, low + bit * half, low + (1 - bit) * half))
        low, size = low + bit * half, half

    def labels_of(source, h, d):
        return jnp.concatenate(
            [
                jnp.broadcast_to(source[h, d, pl.ds(depth + j, 1), :].astype(F32), (rank, part))
                for j in range(most)
            ],
            axis=0,
        ).astype(BF16)

    def part_of(right, source, labels, h, d, c):
        label = jnp.asarray(c, jnp.int32).astype(F32).astype(BF16)
        picked = jnp.where(
            labels == label, source[h, d, pl.ds(0, depth), :], jnp.zeros((), BF16)
        )
        return jnp.dot(right[d], picked, preferred_element_type=F32)

    pl.semaphore_wait(barrier, owners + reps - 2)

    @pl.loop(0, peers)
    def _(k):
        d = turn(k)
        pack(d, vsend, peer(d))
        v_copy(d).start()

    halos = halo_copies()
    for copy in halos:
        copy.start()

    @pl.loop(0, peers)
    def _(k):
        d = turn(k)
        coeffs(d, csend, peer(d))
        c_copy(0, d).start()

    for h in range(1, PARTS):
        @pl.loop(0, peers)
        def _(k):
            c_copy(h, turn(k)).start()

    pack(0, vrecv, row)
    coeffs(0, crecv, row)

    def put(c, value):
        for h in range(PARTS):
            total[h, c] = value[:, h * part:(h + 1) * part]

    def add(c, value):
        for h in range(PARTS):
            total[h, c] = total[h, c] + value[:, h * part:(h + 1) * part]

    @pl.loop(0, clusters)
    def _(c):
        put(c, dot_rows(near[c, 1], field[c, my_rows, :]))

    @pl.loop(0, clusters - 1)
    def _(c):
        add(c + 1, dot_rows(near[c, 2], field[c, my_rows, :]))
        add(c, dot_rows(near[c + 1, 0], field[c + 1, my_rows, :]))

    for copy in halos:
        copy.wait_recv()
    add(0, dot_rows(hnear[0], hfield[0]))
    add(clusters - 1, dot_rows(hnear[1], hfield[1]))

    def far(h, d):
        if h == 0:
            vtr[d] = vrecv[d].T
        labels = labels_of(crecv, h, d)

        @pl.loop(0, clusters)
        def _(c):
            total[h, c] = total[h, c] + part_of(vtr, crecv, labels, h, d, c)

    def far_span(h, first, last):
        @pl.loop(first, last)
        def _(k):
            d = turn(peers - 1 - k)
            if h == 0:
                v_copy(d).wait_recv()
            c_copy(h, d).wait_recv()
            far(h, d)

    def r_copy(h, t):
        return pltpu.make_async_remote_copy(
            src_ref=rsend[t].at[h], dst_ref=rrecv[t].at[h],
            send_sem=rs.at[h, t], recv_sem=rr.at[h, t],
            device_id=(row, plan[t][1]), device_id_type=MESH,
        )

    def g_copy(h, t):
        half, partner, keep, _ = plan[t]
        block = out.at[pl.ds(keep, half), :, pl.ds(h * part, part)]
        return pltpu.make_async_remote_copy(
            src_ref=block, dst_ref=block, send_sem=gs.at[h, t], recv_sem=gr.at[h, t],
            device_id=(row, partner), device_id_type=MESH,
        )

    def give(h, t):
        half, _, _, away = plan[t]

        @pl.loop(0, half)
        def _(i):
            rsend[t][h, i] = total[h, away + i].astype(rsend[t].dtype)

        r_copy(h, t).start()

    def take(h, t):
        half, _, keep, _ = plan[t]
        r_copy(h, t).wait_recv()

        @pl.loop(0, half)
        def _(i):
            value = total[h, keep + i] + rrecv[t][h, i].astype(F32)
            if t == stages - 1:
                out[keep + i, :, pl.ds(h * part, part)] = value.astype(BF16)
            else:
                total[h, keep + i] = value

    def sequence(h):
        steps = [lambda: give(h, 0)]
        for t in range(stages):
            if t < stages - 1:
                steps.append(lambda t=t: (take(h, t), give(h, t + 1)))
            else:
                steps.append(lambda t=t: (take(h, t), g_copy(h, t).start()))
        for t in range(stages - 1, 0, -1):
            steps.append(lambda t=t: (g_copy(h, t).wait_recv(), g_copy(h, t - 1).start()))
        steps.append(lambda: g_copy(h, 0).wait_recv())
        return steps

    ahead, behind = sequence(0), sequence(1)
    far(0, 0)
    far_span(0, 0, peers)
    ahead[0]()
    for step in ahead[1:stages]:
        step()
    middle = peers // 2
    far(1, 0)
    far_span(1, 0, middle)
    ahead[stages]()
    far_span(1, middle, peers)
    behind[0]()
    later = ahead[stages + 1:]
    for place, step in enumerate(behind[1:]):
        if place < len(later):
            later[place]()
        step()

    @pl.loop(1, group)
    def _(d):
        v_copy(d).wait_send()
        for h in range(PARTS):
            c_copy(h, d).wait_send()

    for copy in halos:
        copy.wait_send()
    for h in range(PARTS):
        for t in range(stages):
            r_copy(h, t).wait_send()
            g_copy(h, t).wait_send()


def cube(
    most, facts_hbm, field_hbm, ut_hbm, vt_hbm, near_hbm, out,
    facts, field, ut, vt, near,
    cnat, vsend, csend, vrecv, crecv, vown, cown, vtr, labels, hnear, hfield, total, acc,
    ksend, krecv, qrecv, gsend, grecv, ysend, yrecv, zsend, zrecv,
    xsend, xrecv, fsend, frecv,
    ins, vs, vr, cs, cr, hs, hr, ks, kr, qs, qr, gs, gr, ys, yr, zs, zr, xs, xr, fs, fr, os, orr,
):
    owners, reps = lax.axis_size("rows"), lax.axis_size("rep")
    row, rep = lax.axis_index("rows"), lax.axis_index("rep")
    half = owners // 2
    w, u, y = row // half, lax.rem(row // 2, 2), lax.rem(row, 2)
    x, core = rep // 2, lax.rem(rep, 2)
    blocks, rank, width = ut.shape
    clusters, _, columns = field.shape
    share = near.shape[2]
    depth = most * rank
    pad = vsend.shape[1] - depth
    quad = clusters // 2
    pair = clusters // 4
    sub = width // SPLIT
    bits_of = (blocks - 1).bit_length()

    def at(w_, u_, y_):
        return w_ * half + u_ * 2 + y_

    def mix(t, one, two):
        return one * (1 - t) + two * t

    to_y = (at(w, u, 1 - y), rep)
    to_z = (at(w, 1 - u, y), rep)
    to_x = (row, (1 - x) * 2 + core)
    to_core = (row, x * 2 + 1 - core)
    to_across = (at(1 - w, u, y), rep)
    to_next = (lax.rem(row + mix(y, owners - 2, 2), owners), rep)
    to_prior = (lax.rem(row + mix(y, 2, owners - 2), owners), rep)
    partners = (to_y, to_z, to_x, to_core, to_across, to_next, to_prior)

    barrier = pltpu.get_barrier_semaphore()
    for where in partners:
        pl.semaphore_signal(barrier, inc=1, device_id=where, device_id_type=MESH)

    loads = [
        pltpu.make_async_copy(src, dst, ins.at[i])
        for i, (src, dst) in enumerate(
            (
                (facts_hbm, facts), (vt_hbm, vt), (ut_hbm, ut),
                (field_hbm, field), (near_hbm, near),
            )
        )
    ]
    for load in loads[:2]:
        load.start()

    sends = (
        (to_y, at(1 - w, 1 - u, 1 - y)),
        (to_y, at(1 - w, u, 1 - y)),
        (to_z, at(w, 1 - u, 1 - y)),
        (to_z, at(w, 1 - u, y)),
    )
    owns = (at(1 - w, 1 - u, y), at(1 - w, u, y), at(w, u, 1 - y), row)
    mine = core * quad
    theirs = (1 - core) * quad

    def remote(src, dst, send, recv, where):
        return pltpu.make_async_remote_copy(
            src_ref=src, dst_ref=dst, send_sem=send, recv_sem=recv,
            device_id=where, device_id_type=MESH,
        )

    def v_copy(i):
        return remote(vsend.at[i], vrecv.at[i], vs.at[i], vr.at[i], sends[i][0])

    def c_copy(i):
        return remote(csend.at[i], crecv.at[i], cs.at[i], cr.at[i], sends[i][0])

    def k_copy(i, n):
        return remote(ksend.at[i, n], krecv.at[i, n], ks.at[i, n], kr.at[i, n], to_core)

    def q_copy(n):
        return remote(total.at[theirs + n], qrecv.at[n], qs.at[n], qr.at[n], to_core)

    def g_copy(i, m):
        return remote(gsend.at[i, m], grecv.at[i, m], gs.at[i, m], gr.at[i, m], to_x)

    def y_copy(n):
        return remote(ysend.at[n], yrecv.at[n], ys.at[n], yr.at[n], to_y)

    def z_copy(m):
        return remote(zsend.at[m], zrecv.at[m], zs.at[m], zr.at[m], to_z)

    def x_copy(m):
        return remote(xsend.at[m], xrecv.at[m], xs.at[m], xr.at[m], to_across)

    def f_copy(m):
        return remote(fsend.at[m], frecv.at[m], fs.at[m], fr.at[m], to_x)

    def o_copy(m):
        block = out.at[(mine + x * pair) * SPLIT + m]
        return remote(block, block, os.at[m], orr.at[m], to_x)

    def p_copy(n):
        block = out.at[mine * SPLIT + n]
        spot = pair * SPLIT + n
        return remote(block, block, os.at[spot], orr.at[spot], to_core)

    def note(b, held):
        listed, counts = held[:owners], held[owners:]
        target = facts[0, b]
        hits = [target == o for o in range(owners)]
        return (
            *[jnp.where(hit, old * blocks + b, old) for hit, old in zip(hits, listed)],
            *[jnp.where(hit, old + 1, old) for hit, old in zip(hits, counts)],
        )

    loads[0].wait()
    noted = (jnp.int32(0),) * (2 * owners)
    for b in range(blocks):
        noted = note(b, noted)

    def slots_for(owner):
        listed, count = noted[0], noted[owners]
        for o in range(1, owners):
            listed = jnp.where(owner == o, noted[o], listed)
            count = jnp.where(owner == o, noted[owners + o], count)
        found = []
        for j in range(most):
            found.append((listed & (blocks - 1), j < count))
            listed = listed >> bits_of
        return found

    def pack_v(owner, put):
        lines = lax.broadcasted_iota(jnp.int32, (pad, width), 0)
        marks = jnp.full((pad, width), clusters, jnp.int32)
        for j, (block, valid) in enumerate(slots_for(owner)):
            put(pl.ds(j * rank, rank), vt[block])
            label = jnp.where(valid, facts[1, block], clusters)
            marks = jnp.where(lines == j, label, marks)
        put(pl.ds(depth, pad), marks.astype(F32).astype(BF16))

    def pack_c(owner, put):
        for j, (block, _) in enumerate(slots_for(owner)):
            put(pl.ds(j * rank, rank), cnat[block])

    def send_v(i):
        def put(spot, value):
            vsend[i, spot, :] = value

        pack_v(sends[i][1], put)

    def send_c(i):
        def put(spot, value):
            csend[i, spot, :] = value

        pack_c(sends[i][1], put)
        c_copy(i).start()

    my_rows = pl.ds(pl.multiple_of(rep * share, share), share)
    last = clusters - 1
    halos = [
        remote(near.at[y * last, y * 2], hnear, hs.at[0], hr.at[0], to_next),
        remote(field.at[y * last, my_rows, :], hfield, hs.at[1], hr.at[1], to_next),
    ]

    loads[1].wait()
    for load in loads[2:]:
        load.start()
    send_v(0)
    pl.semaphore_wait(barrier, len(partners))
    v_copy(0).start()
    send_v(2)
    v_copy(2).start()
    for i in (1, 3):
        send_v(i)
    for load in loads[2:]:
        load.wait()
    for copy in halos:
        copy.start()

    def coefficients(b):
        value = jnp.dot(ut[b], field[facts[2, b]], preferred_element_type=F32)
        kept = lax.broadcasted_iota(jnp.int32, (rank, columns), 0) < facts[3, b]
        cnat[b] = jnp.where(kept, value, 0.0).astype(BF16)

    @pl.loop(0, blocks // 4)
    def _(b):
        for e in range(4):
            coefficients(b * 4 + e)

    for i in (0, 2):
        send_c(i)
    for i in (1, 3):
        v_copy(i).start()
        send_c(i)

    def cut(value):
        return [value[s * sub:(s + 1) * sub] for s in range(SPLIT)]

    def prepare(d, factors):
        vtr[d] = factors[pl.ds(0, depth), :].T
        for j in range(most):
            line = factors[pl.ds(depth + j, 1), pl.ds(0, columns)].astype(F32)
            labels[d, pl.ds(j * rank, rank), :] = (
                jnp.broadcast_to(line, (rank, columns)).astype(BF16)
            )

    def part_of(d, coeffs, c):
        label = jnp.asarray(c, jnp.int32).astype(F32).astype(BF16)
        picked = jnp.where(labels[d] == label, coeffs[...], jnp.zeros((), BF16))
        return jnp.dot(vtr[d], picked, preferred_element_type=F32)

    def own(i):
        def put_v(spot, value):
            vown[spot, :] = value

        def put_c(spot, value):
            cown[spot, :] = value

        pack_v(owns[i], put_v)
        pack_c(owns[i], put_c)
        prepare(2, vown)

        @pl.loop(0, clusters // 2)
        def _(k):
            for e in range(2):
                c = 2 * k + e
                for s, value in enumerate(cut(part_of(2, cown, c))):
                    if i < 3:
                        acc[i, c * SPLIT + s] = value
                    else:
                        total[c, s] = value

    def close(c, offset):
        return dot_rows(near[c, offset], field[c, my_rows, :])

    def raise_total(c, value):
        for s, piece in enumerate(cut(value)):
            total[c, s] = total[c, s] + piece

    def raise_acc(c, value):
        for s, piece in enumerate(cut(value)):
            acc[2, c * SPLIT + s] = acc[2, c * SPLIT + s] + piece

    def near_field():
        @pl.loop(1, last)
        def _(c):
            raise_total(c, close(c, 1) + close(c - 1, 2) + close(c + 1, 0))

        raise_total(0, close(0, 1) + close(1, 0))
        raise_total(last, close(last, 1) + close(last - 1, 2))

    def halo_terms():
        for copy in halos:
            copy.wait_recv()
        raise_acc(y * last, close((1 - y) * last, (1 - y) * 2))
        raise_acc((1 - y) * last, dot_rows(hnear[...], hfield[...]))

    def turn(k):
        side = mix(k // pair, 1 - x, x)
        return side * pair + lax.rem(k, pair)

    def ready(i):
        v_copy(i).wait_recv()
        prepare(SPOTS[i], vrecv.at[i])

    def partial_away(i, first, count):
        @pl.loop(0, count // 2)
        def _(k):
            spots = [turn(first + 2 * k + e) for e in range(2)]
            for n in spots:
                c = theirs + n
                value = part_of(SPOTS[i], crecv.at[i], c)
                if i < 3:
                    for s, piece in enumerate(cut(value)):
                        ksend[i, n, s] = (acc[i, c * SPLIT + s] + piece).astype(BF16)
                else:
                    raise_total(c, value)
            for n in spots:
                if i < 3:
                    k_copy(i, n).start()
                else:
                    q_copy(n).start()

    def partial_keep(i, first, count):
        @pl.loop(0, count // 2)
        def _(k):
            for e in range(2):
                c = mine + turn(first + 2 * k + e)
                value = part_of(SPOTS[i], crecv.at[i], c)
                if i < 3:
                    for s, piece in enumerate(cut(value)):
                        acc[i, c * SPLIT + s] = acc[i, c * SPLIT + s] + piece
                else:
                    raise_total(c, value)

    def summed(i, n, s):
        return acc[i, (mine + n) * SPLIT + s] + krecv[i, n, s].astype(F32)

    def give_g(i):
        partial_keep(i, 0, pair)

        @pl.loop(0, pair)
        def _(m):
            n = (1 - x) * pair + m
            k_copy(i, n).wait_recv()
            for s in range(SPLIT):
                gsend[i, m * SPLIT + s] = summed(i, n, s).astype(BF16)
                g_copy(i, m * SPLIT + s).start()

    def give_y():
        @pl.loop(0, quad)
        def _(k):
            n = turn(k)
            k_copy(2, n).wait_recv()
            for s in range(SPLIT):
                ysend[n, s] = summed(2, n, s).astype(BF16)
            y_copy(n).start()

    def take_k(i):
        @pl.loop(0, pair)
        def _(m):
            k_copy(i, x * pair + m).wait_recv()

    def reduced(i, m, s):
        g_copy(i, m * SPLIT + s).wait_recv()
        return summed(i, x * pair + m, s) + grecv[i, m * SPLIT + s].astype(F32)

    def pass_z(m):
        for s in range(SPLIT):
            zsend[m * SPLIT + s] = reduced(0, m, s).astype(BF16)
            z_copy(m * SPLIT + s).start()

    def pass_x(m):
        for s in range(SPLIT):
            value = reduced(1, m, s)
            z_copy(m * SPLIT + s).wait_recv()
            xsend[m * SPLIT + s] = (value + zrecv[m * SPLIT + s].astype(F32)).astype(BF16)
            x_copy(m * SPLIT + s).start()

    def gathered(n, s):
        return total[mine + n, s] + qrecv[n, s] + yrecv[n, s].astype(F32)

    def pass_f(m):
        n = (1 - x) * pair + m
        q_copy(n).wait_recv()
        y_copy(n).wait_recv()
        for s in range(SPLIT):
            fsend[m * SPLIT + s] = gathered(n, s).astype(BF16)
            f_copy(m * SPLIT + s).start()

    for i in (0, 2):
        own(i)
    ready(0)
    own(1)
    own(3)
    ready(2)
    c_copy(0).wait_recv()
    partial_away(0, 0, pair)
    give_g(0)
    partial_away(0, pair, pair)
    halo_terms()
    c_copy(2).wait_recv()
    partial_away(2, 0, quad)
    partial_keep(2, 0, quad)
    partial_keep(0, pair, pair)
    give_y()
    take_k(0)
    near_field()
    pass_z(0)
    ready(1)
    c_copy(1).wait_recv()
    partial_away(1, 0, pair)
    give_g(1)
    partial_away(1, pair, pair)
    for m in range(1, pair):
        pass_z(m)
    partial_keep(1, pair, pair)
    take_k(1)
    ready(3)
    c_copy(3).wait_recv()
    partial_away(3, 0, quad)
    partial_keep(3, 0, quad)

    @pl.loop(0, pair)
    def _(m):
        pass_f(m)
        pass_x(m)

    @pl.loop(0, pair)
    def _(m):
        n = x * pair + m
        q_copy(n).wait_recv()
        y_copy(n).wait_recv()
        for s in range(SPLIT):
            piece = m * SPLIT + s
            f_copy(piece).wait_recv()
            value = gathered(n, s) + frecv[piece].astype(F32)
            x_copy(piece).wait_recv()
            out[(mine + n) * SPLIT + s] = (value + xrecv[piece].astype(F32)).astype(BF16)
            o_copy(piece).start()
            p_copy(n * SPLIT + s).start()

    @pl.loop(0, pair * SPLIT)
    def _(m):
        o_copy(m).wait_recv()
        p_copy((1 - x) * pair * SPLIT + m).start()

    @pl.loop(0, quad * SPLIT)
    def _(n):
        p_copy(n).wait_recv()
        p_copy(n).wait_send()

    for copy in halos:
        copy.wait_send()
    for i in range(4):
        v_copy(i).wait_send()
        c_copy(i).wait_send()

    @pl.loop(0, quad)
    def _(n):
        for i in range(3):
            k_copy(i, n).wait_send()
        q_copy(n).wait_send()
        y_copy(n).wait_send()

    @pl.loop(0, pair * SPLIT)
    def _(m):
        for i in range(2):
            g_copy(i, m).wait_send()
        z_copy(m).wait_send()
        x_copy(m).wait_send()
        f_copy(m).wait_send()
        o_copy(m).wait_send()


def slots_of(col_owner, owners, most):
    target = col_owner[:, 0]
    number = jnp.arange(target.shape[0], dtype=jnp.int32)
    same = (target[:, None] == target[None, :]) & (number[None, :] < number[:, None])
    slot = target * most + jnp.sum(same.astype(jnp.int32), axis=1)
    return slot[:, None] == jnp.arange(owners * most, dtype=jnp.int32)[None, :]


def table(held, clusters, facts):
    lift = [0] * (len(facts) - 1) + [clusters]
    tab = jnp.sum(jnp.where(held[None], jnp.stack(facts)[:, :, None], 0), axis=1)
    return tab + jnp.array(lift, jnp.int32)[:, None]


def shards(
    field_in,
    left_factors,
    right_factors,
    block_ranks,
    row_cluster,
    col_owner,
    col_cluster,
    near_blocks,
):
    owners, reps = lax.axis_size("rows"), lax.axis_size("rep")
    blocks, width, rank = left_factors.shape
    clusters, _, columns = field_in.shape
    share = near_blocks.shape[2]
    most = 5 * blocks // (4 * owners) + 1
    part = columns // PARTS
    depth = most * rank
    pad = -(-most // 16) * 16
    tall = depth + pad
    stages = reps.bit_length() - 1

    smem = pl.BlockSpec(memory_space=pltpu.SMEM)
    vmem = pl.BlockSpec(memory_space=pltpu.VMEM)
    dma = pltpu.SemaphoreType.DMA
    arrays = (
        field_in,
        jnp.swapaxes(left_factors, 1, 2),
        jnp.swapaxes(right_factors, 1, 2),
        near_blocks,
    )
    cubic = stages == 2 and owners == 2 ** 3 and (blocks - 1).bit_length() * most < 32
    cubic = cubic and blocks == 2 ** (blocks - 1).bit_length()
    cubic = cubic and columns <= width
    if cubic:
        quad, pair = clusters // 2, clusters // 4
        slab = (width // SPLIT, columns)
        keep = pltpu.VMEM
        gathered = pl.pallas_call(
            functools.partial(cube, most),
            out_shape=jax.ShapeDtypeStruct((clusters * SPLIT, *slab), BF16),
            in_specs=[pl.BlockSpec(memory_space=pltpu.HBM)] * 5,
            out_specs=vmem,
            scratch_shapes=[
                pltpu.SMEM((4, blocks), jnp.int32),
                *[keep(array.shape, BF16) for array in arrays],
                keep((blocks, rank, columns), BF16),
                keep((4, tall, width), BF16),
                keep((4, depth, columns), BF16),
                keep((4, tall, width), BF16),
                keep((4, depth, columns), BF16),
                keep((tall, width), BF16),
                keep((depth, columns), BF16),
                keep((3, width, depth), BF16),
                keep((3, depth, columns), BF16),
                keep((share, width), BF16),
                keep((share, columns), BF16),
                keep((clusters, SPLIT, *slab), F32),
                keep((3, clusters * SPLIT, *slab), F32),
                keep((3, quad, SPLIT, *slab), BF16),
                keep((3, quad, SPLIT, *slab), BF16),
                keep((quad, SPLIT, *slab), F32),
                keep((2, pair * SPLIT, *slab), BF16),
                keep((2, pair * SPLIT, *slab), BF16),
                keep((quad, SPLIT, *slab), BF16),
                keep((quad, SPLIT, *slab), BF16),
                *[keep((pair * SPLIT, *slab), BF16)] * 6,
                dma((5,)),
                *[dma((4,))] * 6,
                *[dma((3, quad))] * 2,
                *[dma((quad,))] * 2,
                *[dma((2, pair * SPLIT))] * 2,
                *[dma((quad,))] * 2,
                *[dma((pair * SPLIT,))] * 6,
                *[dma(((pair + quad) * SPLIT,))] * 2,
            ],
            compiler_params=pltpu.CompilerParams(
                collective_id=0, has_side_effects=True, vmem_limit_bytes=52 * 1024 * 1024
            ),
        )(jnp.stack([col_owner[:, 0], col_cluster, row_cluster, block_ranks]), *arrays)
        return gathered.reshape(field_in.shape).astype(F32)

    held = slots_of(col_owner, owners, most)
    number = jnp.arange(blocks, dtype=jnp.int32)
    halves = [clusters >> (t + 1) for t in range(stages)]
    steps = [
        pltpu.VMEM((PARTS, half, width, part), BF16 if t else F32) for t, half in enumerate(halves)
    ]
    gathered = pl.pallas_call(
        functools.partial(kernel, owners, reps, most),
        out_shape=jax.ShapeDtypeStruct(field_in.shape, BF16),
        in_specs=[smem] + [vmem] * 4,
        out_specs=vmem,
        scratch_shapes=[
            pltpu.VMEM((owners, depth, width), BF16),
            pltpu.VMEM((owners, depth, width), BF16),
            pltpu.VMEM((owners, width, depth), BF16),
            pltpu.VMEM((PARTS, owners, tall, part), BF16),
            pltpu.VMEM((PARTS, owners, tall, part), BF16),
            pltpu.VMEM((2, share, width), BF16),
            pltpu.VMEM((2, share, columns), BF16),
            pltpu.VMEM((PARTS, clusters, width, part), F32),
            *steps,
            *steps,
            dma((owners,)),
            dma((owners,)),
            dma((PARTS, owners)),
            dma((PARTS, owners)),
            dma((4,)),
            dma((4,)),
            *[dma((PARTS, stages))] * 4,
        ],
        compiler_params=pltpu.CompilerParams(
            collective_id=0, has_side_effects=True, vmem_limit_bytes=60 * 1024 * 1024
        ),
    )(table(held, clusters, [number, row_cluster, block_ranks, col_cluster - clusters]), *arrays)
    return gathered.astype(F32)


def solution(mesh):
    in_specs = (
        P("rows", None, None),
        P(("rows", "rep"), None, None),
        P(("rows", "rep"), None, None),
        P(("rows", "rep")),
        P(("rows", "rep")),
        P(("rows", "rep"), None),
        P(("rows", "rep")),
        P("rows", None, "rep", None),
    )
    out_specs = P("rows", None, None)
    return jax.shard_map(shards, mesh=mesh, in_specs=in_specs, out_specs=out_specs, check_vma=False)
```

```python
import functools

import jax
import jax.numpy as jnp
from jax import lax
from jax.experimental import pallas as pl
from jax.experimental.pallas import tpu as pltpu
from jax.sharding import PartitionSpec as P

MESH = pl.DeviceIdType.MESH
PARTS = 2
SPLIT = 2
SPOTS = (0, 0, 1, 1)
BF16 = jnp.bfloat16
F32 = jnp.float32


def dot_rows(left, right):
    return lax.dot_general(left, right, (((0,), (0,)), ((), ())), preferred_element_type=F32)


def kernel(
    owners, reps, most, tab, field, ut, vt, near, out,
    vsend, vrecv, vtr, csend, crecv, hnear, hfield, total, *rest,
):
    stages = reps.bit_length() - 1
    rsend, rrecv = rest[:stages], rest[stages:2 * stages]
    vs, vr, cs, cr, hs, hr, rs, rr, gs, gr = rest[2 * stages:]
    group = owners
    row, rep = lax.axis_index("rows"), lax.axis_index("rep")
    place_in = lax.rem(row, group)
    base = row - place_in
    blocks, rank, width = ut.shape
    clusters, _, columns = field.shape
    share = near.shape[2]
    part = columns // PARTS
    depth = most * rank
    peers = group - 1

    barrier = pltpu.get_barrier_semaphore()

    @pl.loop(1, owners)
    def _(d):
        pl.semaphore_signal(
            barrier, inc=1, device_id=(lax.rem(row + d, owners), rep), device_id_type=MESH
        )

    @pl.loop(1, reps)
    def _(d):
        pl.semaphore_signal(
            barrier, inc=1, device_id=(row, lax.rem(rep + d, reps)), device_id_type=MESH
        )

    def peer(d):
        return base + lax.rem(place_in + d, group)

    def turn(k):
        step = (k + 1) // 2
        return group // 2 + lax.rem(k, 2) * step - (1 - lax.rem(k, 2)) * step

    def v_copy(d):
        return pltpu.make_async_remote_copy(
            src_ref=vsend.at[d], dst_ref=vrecv.at[d], send_sem=vs.at[d], recv_sem=vr.at[d],
            device_id=(peer(d), rep), device_id_type=MESH,
        )

    def c_copy(h, d):
        return pltpu.make_async_remote_copy(
            src_ref=csend.at[h, d], dst_ref=crecv.at[h, d],
            send_sem=cs.at[h, d], recv_sem=cr.at[h, d],
            device_id=(peer(d), rep), device_id_type=MESH,
        )

    def pack(d, target, owner):
        for j in range(most):
            target[d, pl.ds(j * rank, rank), :] = vt[tab[0, owner * most + j]]

    def coeffs(d, target, owner):
        extra = csend.shape[2] - depth
        lines = lax.broadcasted_iota(jnp.int32, (extra, part), 0)
        marks = jnp.full((extra, part), clusters, jnp.int32)
        for j in range(most):
            slot = owner * most + j
            value = jnp.dot(ut[tab[0, slot]], field[tab[1, slot]], preferred_element_type=F32)
            kept = lax.broadcasted_iota(jnp.int32, (rank, columns), 0) < tab[2, slot]
            value = jnp.where(kept, value, 0.0).astype(BF16)
            for h in range(PARTS):
                target[h, d, pl.ds(j * rank, rank), :] = value[:, h * part:(h + 1) * part]
            marks = jnp.where(lines == j, tab[3, slot], marks)
        for h in range(PARTS):
            target[h, d, pl.ds(depth, extra), :] = marks.astype(F32).astype(BF16)

    my_rows = pl.ds(pl.multiple_of(rep * share, share), share)

    def halo_copies():
        made = []
        for side, cluster, offset, shift in ((0, clusters - 1, 2, 1), (1, 0, 0, owners - 1)):
            where = (lax.rem(row + shift, owners), rep)
            made.append(pltpu.make_async_remote_copy(
                src_ref=near.at[cluster, offset], dst_ref=hnear.at[side],
                send_sem=hs.at[2 * side], recv_sem=hr.at[2 * side],
                device_id=where, device_id_type=MESH,
            ))
            made.append(pltpu.make_async_remote_copy(
                src_ref=field.at[cluster, my_rows, :], dst_ref=hfield.at[side],
                send_sem=hs.at[2 * side + 1], recv_sem=hr.at[2 * side + 1],
                device_id=where, device_id_type=MESH,
            ))
        return made

    plan = []
    low, size = 0, clusters
    for t in range(stages):
        bit = lax.rem(rep // (1 << t), 2)
        half = size // 2
        partner = rep + (1 << t) * (1 - 2 * bit)
        plan.append((half, partner, low + bit * half, low + (1 - bit) * half))
        low, size = low + bit * half, half

    def labels_of(source, h, d):
        return jnp.concatenate(
            [
                jnp.broadcast_to(source[h, d, pl.ds(depth + j, 1), :].astype(F32), (rank, part))
                for j in range(most)
            ],
            axis=0,
        ).astype(BF16)

    def part_of(right, source, labels, h, d, c):
        label = jnp.asarray(c, jnp.int32).astype(F32).astype(BF16)
        picked = jnp.where(
            labels == label, source[h, d, pl.ds(0, depth), :], jnp.zeros((), BF16)
        )
        return jnp.dot(right[d], picked, preferred_element_type=F32)

    pl.semaphore_wait(barrier, owners + reps - 2)

    @pl.loop(0, peers)
    def _(k):
        d = turn(k)
        pack(d, vsend, peer(d))
        v_copy(d).start()

    halos = halo_copies()
    for copy in halos:
        copy.start()

    @pl.loop(0, peers)
    def _(k):
        d = turn(k)
        coeffs(d, csend, peer(d))
        c_copy(0, d).start()

    for h in range(1, PARTS):
        @pl.loop(0, peers)
        def _(k):
            c_copy(h, turn(k)).start()

    pack(0, vrecv, row)
    coeffs(0, crecv, row)

    def put(c, value):
        for h in range(PARTS):
            total[h, c] = value[:, h * part:(h + 1) * part]

    def add(c, value):
        for h in range(PARTS):
            total[h, c] = total[h, c] + value[:, h * part:(h + 1) * part]

    @pl.loop(0, clusters)
    def _(c):
        put(c, dot_rows(near[c, 1], field[c, my_rows, :]))

    @pl.loop(0, clusters - 1)
    def _(c):
        add(c + 1, dot_rows(near[c, 2], field[c, my_rows, :]))
        add(c, dot_rows(near[c + 1, 0], field[c + 1, my_rows, :]))

    for copy in halos:
        copy.wait_recv()
    add(0, dot_rows(hnear[0], hfield[0]))
    add(clusters - 1, dot_rows(hnear[1], hfield[1]))

    def far(h, d):
        if h == 0:
            vtr[d] = vrecv[d].T
        labels = labels_of(crecv, h, d)

        @pl.loop(0, clusters)
        def _(c):
            total[h, c] = total[h, c] + part_of(vtr, crecv, labels, h, d, c)

    def far_span(h, first, last):
        @pl.loop(first, last)
        def _(k):
            d = turn(peers - 1 - k)
            if h == 0:
                v_copy(d).wait_recv()
            c_copy(h, d).wait_recv()
            far(h, d)

    def r_copy(h, t):
        return pltpu.make_async_remote_copy(
            src_ref=rsend[t].at[h], dst_ref=rrecv[t].at[h],
            send_sem=rs.at[h, t], recv_sem=rr.at[h, t],
            device_id=(row, plan[t][1]), device_id_type=MESH,
        )

    def g_copy(h, t):
        half, partner, keep, _ = plan[t]
        block = out.at[pl.ds(keep, half), :, pl.ds(h * part, part)]
        return pltpu.make_async_remote_copy(
            src_ref=block, dst_ref=block, send_sem=gs.at[h, t], recv_sem=gr.at[h, t],
            device_id=(row, partner), device_id_type=MESH,
        )

    def give(h, t):
        half, _, _, away = plan[t]

        @pl.loop(0, half)
        def _(i):
            rsend[t][h, i] = total[h, away + i].astype(rsend[t].dtype)

        r_copy(h, t).start()

    def take(h, t):
        half, _, keep, _ = plan[t]
        r_copy(h, t).wait_recv()

        @pl.loop(0, half)
        def _(i):
            value = total[h, keep + i] + rrecv[t][h, i].astype(F32)
            if t == stages - 1:
                out[keep + i, :, pl.ds(h * part, part)] = value.astype(BF16)
            else:
                total[h, keep + i] = value

    def sequence(h):
        steps = [lambda: give(h, 0)]
        for t in range(stages):
            if t < stages - 1:
                steps.append(lambda t=t: (take(h, t), give(h, t + 1)))
            else:
                steps.append(lambda t=t: (take(h, t), g_copy(h, t).start()))
        for t in range(stages - 1, 0, -1):
            steps.append(lambda t=t: (g_copy(h, t).wait_recv(), g_copy(h, t - 1).start()))
        steps.append(lambda: g_copy(h, 0).wait_recv())
        return steps

    ahead, behind = sequence(0), sequence(1)
    far(0, 0)
    far_span(0, 0, peers)
    ahead[0]()
    for step in ahead[1:stages]:
        step()
    middle = peers // 2
    far(1, 0)
    far_span(1, 0, middle)
    ahead[stages]()
    far_span(1, middle, peers)
    behind[0]()
    later = ahead[stages + 1:]
    for place, step in enumerate(behind[1:]):
        if place < len(later):
            later[place]()
        step()

    @pl.loop(1, group)
    def _(d):
        v_copy(d).wait_send()
        for h in range(PARTS):
            c_copy(h, d).wait_send()

    for copy in halos:
        copy.wait_send()
    for h in range(PARTS):
        for t in range(stages):
            r_copy(h, t).wait_send()
            g_copy(h, t).wait_send()


def cube(
    most, facts_hbm, field_hbm, ut_hbm, vt_hbm, near_hbm, out,
    facts, field, ut, vt, near,
    cnat, vsend, csend, vrecv, crecv, vown, cown, vtr, labels, hnear, hfield, total, acc,
    ksend, krecv, qrecv, gsend, grecv, ysend, yrecv, zsend, zrecv,
    xsend, xrecv, fsend, frecv,
    ins, vs, vr, cs, cr, hs, hr, ks, kr, qs, qr, gs, gr, ys, yr, zs, zr, xs, xr, fs, fr, os, orr,
):
    owners, reps = lax.axis_size("rows"), lax.axis_size("rep")
    row, rep = lax.axis_index("rows"), lax.axis_index("rep")
    half = owners // 2
    w, u, y = row // half, lax.rem(row // 2, 2), lax.rem(row, 2)
    x, core = rep // 2, lax.rem(rep, 2)
    blocks, rank, width = ut.shape
    clusters, _, columns = field.shape
    share = near.shape[2]
    depth = most * rank
    pad = vsend.shape[1] - depth
    quad = clusters // 2
    pair = clusters // 4
    sub = width // SPLIT
    bits_of = (blocks - 1).bit_length()

    def at(w_, u_, y_):
        return w_ * half + u_ * 2 + y_

    def mix(t, one, two):
        return one * (1 - t) + two * t

    to_y = (at(w, u, 1 - y), rep)
    to_z = (at(w, 1 - u, y), rep)
    to_x = (row, (1 - x) * 2 + core)
    to_core = (row, x * 2 + 1 - core)
    to_across = (at(1 - w, u, y), rep)
    to_next = (lax.rem(row + mix(y, owners - 2, 2), owners), rep)
    to_prior = (lax.rem(row + mix(y, 2, owners - 2), owners), rep)
    partners = (to_y, to_z, to_x, to_core, to_across, to_next, to_prior)

    barrier = pltpu.get_barrier_semaphore()
    for where in partners:
        pl.semaphore_signal(barrier, inc=1, device_id=where, device_id_type=MESH)

    loads = [
        pltpu.make_async_copy(src, dst, ins.at[i])
        for i, (src, dst) in enumerate(
            (
                (facts_hbm, facts), (vt_hbm, vt), (ut_hbm, ut),
                (field_hbm, field), (near_hbm, near),
            )
        )
    ]
    for load in loads[:2]:
        load.start()

    sends = (
        (to_y, at(1 - w, 1 - u, 1 - y)),
        (to_y, at(1 - w, u, 1 - y)),
        (to_z, at(w, 1 - u, 1 - y)),
        (to_z, at(w, 1 - u, y)),
    )
    owns = (at(1 - w, 1 - u, y), at(1 - w, u, y), at(w, u, 1 - y), row)
    mine = core * quad
    theirs = (1 - core) * quad

    def remote(src, dst, send, recv, where):
        return pltpu.make_async_remote_copy(
            src_ref=src, dst_ref=dst, send_sem=send, recv_sem=recv,
            device_id=where, device_id_type=MESH,
        )

    def v_copy(i):
        return remote(vsend.at[i], vrecv.at[i], vs.at[i], vr.at[i], sends[i][0])

    def c_copy(i):
        return remote(csend.at[i], crecv.at[i], cs.at[i], cr.at[i], sends[i][0])

    def k_copy(i, n):
        return remote(ksend.at[i, n], krecv.at[i, n], ks.at[i, n], kr.at[i, n], to_core)

    def q_copy(n):
        return remote(total.at[theirs + n], qrecv.at[n], qs.at[n], qr.at[n], to_core)

    def g_copy(i, m):
        return remote(gsend.at[i, m], grecv.at[i, m], gs.at[i, m], gr.at[i, m], to_x)

    def y_copy(n):
        return remote(ysend.at[n], yrecv.at[n], ys.at[n], yr.at[n], to_y)

    def z_copy(m):
        return remote(zsend.at[m], zrecv.at[m], zs.at[m], zr.at[m], to_z)

    def x_copy(m):
        return remote(xsend.at[m], xrecv.at[m], xs.at[m], xr.at[m], to_across)

    def f_copy(m):
        return remote(fsend.at[m], frecv.at[m], fs.at[m], fr.at[m], to_x)

    def o_copy(m):
        block = out.at[(mine + x * pair) * SPLIT + m]
        return remote(block, block, os.at[m], orr.at[m], to_x)

    def p_copy(n):
        block = out.at[mine * SPLIT + n]
        spot = pair * SPLIT + n
        return remote(block, block, os.at[spot], orr.at[spot], to_core)

    def note(b, held):
        listed, counts = held[:owners], held[owners:]
        target = facts[0, b]
        hits = [target == o for o in range(owners)]
        return (
            *[jnp.where(hit, old * blocks + b, old) for hit, old in zip(hits, listed)],
            *[jnp.where(hit, old + 1, old) for hit, old in zip(hits, counts)],
        )

    loads[0].wait()
    noted = (jnp.int32(0),) * (2 * owners)
    for b in range(blocks):
        noted = note(b, noted)

    def slots_for(owner):
        listed, count = noted[0], noted[owners]
        for o in range(1, owners):
            listed = jnp.where(owner == o, noted[o], listed)
            count = jnp.where(owner == o, noted[owners + o], count)
        found = []
        for j in range(most):
            found.append((listed & (blocks - 1), j < count))
            listed = listed >> bits_of
        return found

    def pack_v(owner, put):
        lines = lax.broadcasted_iota(jnp.int32, (pad, width), 0)
        marks = jnp.full((pad, width), clusters, jnp.int32)
        for j, (block, valid) in enumerate(slots_for(owner)):
            put(pl.ds(j * rank, rank), vt[block])
            label = jnp.where(valid, facts[1, block], clusters)
            marks = jnp.where(lines == j, label, marks)
        put(pl.ds(depth, pad), marks.astype(F32).astype(BF16))

    def pack_c(owner, put):
        for j, (block, _) in enumerate(slots_for(owner)):
            put(pl.ds(j * rank, rank), cnat[block])

    def send_v(i):
        def put(spot, value):
            vsend[i, spot, :] = value

        pack_v(sends[i][1], put)

    def send_c(i):
        def put(spot, value):
            csend[i, spot, :] = value

        pack_c(sends[i][1], put)
        c_copy(i).start()

    my_rows = pl.ds(pl.multiple_of(rep * share, share), share)
    last = clusters - 1
    halos = [
        remote(near.at[y * last, y * 2], hnear, hs.at[0], hr.at[0], to_next),
        remote(field.at[y * last, my_rows, :], hfield, hs.at[1], hr.at[1], to_next),
    ]

    loads[1].wait()
    for load in loads[2:]:
        load.start()
    send_v(0)
    pl.semaphore_wait(barrier, len(partners))
    v_copy(0).start()
    send_v(2)
    v_copy(2).start()
    for i in (1, 3):
        send_v(i)
    for load in loads[2:4]:
        load.wait()

    def coefficients(b):
        value = jnp.dot(ut[b], field[facts[2, b]], preferred_element_type=F32)
        kept = lax.broadcasted_iota(jnp.int32, (rank, columns), 0) < facts[3, b]
        cnat[b] = jnp.where(kept, value, 0.0).astype(BF16)

    @pl.loop(0, blocks // 4)
    def _(b):
        for e in range(4):
            coefficients(b * 4 + e)

    send_c(0)
    loads[4].wait()
    for copy in halos:
        copy.start()
    send_c(2)
    for i in (1, 3):
        v_copy(i).start()
        send_c(i)

    def cut(value):
        return [value[s * sub:(s + 1) * sub] for s in range(SPLIT)]

    def prepare(d, factors):
        vtr[d] = factors[pl.ds(0, depth), :].T
        for j in range(most):
            line = factors[pl.ds(depth + j, 1), pl.ds(0, columns)].astype(F32)
            labels[d, pl.ds(j * rank, rank), :] = (
                jnp.broadcast_to(line, (rank, columns)).astype(BF16)
            )

    def part_of(d, coeffs, c):
        label = jnp.asarray(c, jnp.int32).astype(F32).astype(BF16)
        picked = jnp.where(labels[d] == label, coeffs[...], jnp.zeros((), BF16))
        return jnp.dot(vtr[d], picked, preferred_element_type=F32)

    def own(i):
        def put_v(spot, value):
            vown[spot, :] = value

        def put_c(spot, value):
            cown[spot, :] = value

        pack_v(owns[i], put_v)
        pack_c(owns[i], put_c)
        prepare(2, vown)

        @pl.loop(0, clusters // 2)
        def _(k):
            for e in range(2):
                c = 2 * k + e
                for s, value in enumerate(cut(part_of(2, cown, c))):
                    if i < 3:
                        acc[i, c * SPLIT + s] = value
                    else:
                        total[c, s] = value

    def close(c, offset):
        return dot_rows(near[c, offset], field[c, my_rows, :])

    def raise_total(c, value):
        for s, piece in enumerate(cut(value)):
            total[c, s] = total[c, s] + piece

    def raise_acc(c, value):
        for s, piece in enumerate(cut(value)):
            acc[2, c * SPLIT + s] = acc[2, c * SPLIT + s] + piece

    def near_field():
        @pl.loop(1, last)
        def _(c):
            raise_total(c, close(c, 1) + close(c - 1, 2) + close(c + 1, 0))

        raise_total(0, close(0, 1) + close(1, 0))
        raise_total(last, close(last, 1) + close(last - 1, 2))

    def halo_terms():
        for copy in halos:
            copy.wait_recv()
        raise_acc(y * last, close((1 - y) * last, (1 - y) * 2))
        raise_acc((1 - y) * last, dot_rows(hnear[...], hfield[...]))

    def turn(k):
        side = mix(k // pair, 1 - x, x)
        return side * pair + lax.rem(k, pair)

    def ready(i):
        v_copy(i).wait_recv()
        prepare(SPOTS[i], vrecv.at[i])

    def partial_away(i, first, count):
        @pl.loop(0, count // 2)
        def _(k):
            spots = [turn(first + 2 * k + e) for e in range(2)]
            for n in spots:
                c = theirs + n
                value = part_of(SPOTS[i], crecv.at[i], c)
                if i < 3:
                    for s, piece in enumerate(cut(value)):
                        ksend[i, n, s] = (acc[i, c * SPLIT + s] + piece).astype(BF16)
                else:
                    raise_total(c, value)
            for n in spots:
                if i < 3:
                    k_copy(i, n).start()
                else:
                    q_copy(n).start()

    def partial_keep(i, first, count):
        @pl.loop(0, count // 2)
        def _(k):
            for e in range(2):
                c = mine + turn(first + 2 * k + e)
                value = part_of(SPOTS[i], crecv.at[i], c)
                if i < 3:
                    for s, piece in enumerate(cut(value)):
                        acc[i, c * SPLIT + s] = acc[i, c * SPLIT + s] + piece
                else:
                    raise_total(c, value)

    def summed(i, n, s):
        return acc[i, (mine + n) * SPLIT + s] + krecv[i, n, s].astype(F32)

    def give_g(i):
        partial_keep(i, 0, pair)

        @pl.loop(0, pair)
        def _(m):
            n = (1 - x) * pair + m
            k_copy(i, n).wait_recv()
            for s in range(SPLIT):
                gsend[i, m * SPLIT + s] = summed(i, n, s).astype(BF16)
                g_copy(i, m * SPLIT + s).start()

    def give_y():
        @pl.loop(0, quad)
        def _(k):
            n = turn(k)
            k_copy(2, n).wait_recv()
            for s in range(SPLIT):
                ysend[n, s] = summed(2, n, s).astype(BF16)
            y_copy(n).start()

    def take_k(i):
        @pl.loop(0, pair)
        def _(m):
            k_copy(i, x * pair + m).wait_recv()

    def reduced(i, m, s):
        g_copy(i, m * SPLIT + s).wait_recv()
        return summed(i, x * pair + m, s) + grecv[i, m * SPLIT + s].astype(F32)

    def pass_z(m):
        for s in range(SPLIT):
            zsend[m * SPLIT + s] = reduced(0, m, s).astype(BF16)
            z_copy(m * SPLIT + s).start()

    def pass_x(m):
        for s in range(SPLIT):
            value = reduced(1, m, s)
            z_copy(m * SPLIT + s).wait_recv()
            xsend[m * SPLIT + s] = (value + zrecv[m * SPLIT + s].astype(F32)).astype(BF16)
            x_copy(m * SPLIT + s).start()

    def gathered(n, s):
        return total[mine + n, s] + qrecv[n, s] + yrecv[n, s].astype(F32)

    def pass_f(m):
        n = (1 - x) * pair + m
        q_copy(n).wait_recv()
        y_copy(n).wait_recv()
        for s in range(SPLIT):
            fsend[m * SPLIT + s] = gathered(n, s).astype(BF16)
            f_copy(m * SPLIT + s).start()

    for i in (0, 2):
        own(i)
    ready(0)
    own(1)
    own(3)
    ready(2)
    c_copy(0).wait_recv()
    partial_away(0, 0, pair)
    give_g(0)
    partial_away(0, pair, pair)
    halo_terms()
    c_copy(2).wait_recv()
    partial_away(2, 0, quad)
    partial_keep(2, 0, quad)
    partial_keep(0, pair, pair)
    give_y()
    take_k(0)
    near_field()
    pass_z(0)
    ready(1)
    c_copy(1).wait_recv()
    partial_away(1, 0, pair)
    give_g(1)
    partial_away(1, pair, pair)
    for m in range(1, pair):
        pass_z(m)
    partial_keep(1, pair, pair)
    take_k(1)
    ready(3)
    c_copy(3).wait_recv()
    partial_away(3, 0, quad)
    partial_keep(3, 0, quad)

    @pl.loop(0, pair)
    def _(m):
        pass_f(m)
        pass_x(m)

    @pl.loop(0, pair)
    def _(m):
        n = x * pair + m
        q_copy(n).wait_recv()
        y_copy(n).wait_recv()
        for s in range(SPLIT):
            piece = m * SPLIT + s
            f_copy(piece).wait_recv()
            value = gathered(n, s) + frecv[piece].astype(F32)
            x_copy(piece).wait_recv()
            out[(mine + n) * SPLIT + s] = (value + xrecv[piece].astype(F32)).astype(BF16)
            o_copy(piece).start()
            p_copy(n * SPLIT + s).start()

    @pl.loop(0, pair * SPLIT)
    def _(m):
        o_copy(m).wait_recv()
        p_copy((1 - x) * pair * SPLIT + m).start()

    @pl.loop(0, quad * SPLIT)
    def _(n):
        p_copy(n).wait_recv()
        p_copy(n).wait_send()

    for copy in halos:
        copy.wait_send()
    for i in range(4):
        v_copy(i).wait_send()
        c_copy(i).wait_send()

    @pl.loop(0, quad)
    def _(n):
        for i in range(3):
            k_copy(i, n).wait_send()
        q_copy(n).wait_send()
        y_copy(n).wait_send()

    @pl.loop(0, pair * SPLIT)
    def _(m):
        for i in range(2):
            g_copy(i, m).wait_send()
        z_copy(m).wait_send()
        x_copy(m).wait_send()
        f_copy(m).wait_send()
        o_copy(m).wait_send()


def slots_of(col_owner, owners, most):
    target = col_owner[:, 0]
    number = jnp.arange(target.shape[0], dtype=jnp.int32)
    same = (target[:, None] == target[None, :]) & (number[None, :] < number[:, None])
    slot = target * most + jnp.sum(same.astype(jnp.int32), axis=1)
    return slot[:, None] == jnp.arange(owners * most, dtype=jnp.int32)[None, :]


def table(held, clusters, facts):
    lift = [0] * (len(facts) - 1) + [clusters]
    tab = jnp.sum(jnp.where(held[None], jnp.stack(facts)[:, :, None], 0), axis=1)
    return tab + jnp.array(lift, jnp.int32)[:, None]


def shards(
    field_in,
    left_factors,
    right_factors,
    block_ranks,
    row_cluster,
    col_owner,
    col_cluster,
    near_blocks,
):
    owners, reps = lax.axis_size("rows"), lax.axis_size("rep")
    blocks, width, rank = left_factors.shape
    clusters, _, columns = field_in.shape
    share = near_blocks.shape[2]
    most = 5 * blocks // (4 * owners) + 1
    part = columns // PARTS
    depth = most * rank
    pad = -(-most // 16) * 16
    tall = depth + pad
    stages = reps.bit_length() - 1

    smem = pl.BlockSpec(memory_space=pltpu.SMEM)
    vmem = pl.BlockSpec(memory_space=pltpu.VMEM)
    dma = pltpu.SemaphoreType.DMA
    arrays = (
        field_in,
        jnp.swapaxes(left_factors, 1, 2),
        jnp.swapaxes(right_factors, 1, 2),
        near_blocks,
    )
    cubic = stages == 2 and owners == 2 ** 3 and (blocks - 1).bit_length() * most < 32
    cubic = cubic and blocks == 2 ** (blocks - 1).bit_length()
    cubic = cubic and columns <= width
    if cubic:
        quad, pair = clusters // 2, clusters // 4
        slab = (width // SPLIT, columns)
        keep = pltpu.VMEM
        gathered = pl.pallas_call(
            functools.partial(cube, most),
            out_shape=jax.ShapeDtypeStruct((clusters * SPLIT, *slab), BF16),
            in_specs=[pl.BlockSpec(memory_space=pltpu.HBM)] * 5,
            out_specs=vmem,
            scratch_shapes=[
                pltpu.SMEM((4, blocks), jnp.int32),
                *[keep(array.shape, BF16) for array in arrays],
                keep((blocks, rank, columns), BF16),
                keep((4, tall, width), BF16),
                keep((4, depth, columns), BF16),
                keep((4, tall, width), BF16),
                keep((4, depth, columns), BF16),
                keep((tall, width), BF16),
                keep((depth, columns), BF16),
                keep((3, width, depth), BF16),
                keep((3, depth, columns), BF16),
                keep((share, width), BF16),
                keep((share, columns), BF16),
                keep((clusters, SPLIT, *slab), F32),
                keep((3, clusters * SPLIT, *slab), F32),
                keep((3, quad, SPLIT, *slab), BF16),
                keep((3, quad, SPLIT, *slab), BF16),
                keep((quad, SPLIT, *slab), F32),
                keep((2, pair * SPLIT, *slab), BF16),
                keep((2, pair * SPLIT, *slab), BF16),
                keep((quad, SPLIT, *slab), BF16),
                keep((quad, SPLIT, *slab), BF16),
                *[keep((pair * SPLIT, *slab), BF16)] * 6,
                dma((5,)),
                *[dma((4,))] * 6,
                *[dma((3, quad))] * 2,
                *[dma((quad,))] * 2,
                *[dma((2, pair * SPLIT))] * 2,
                *[dma((quad,))] * 2,
                *[dma((pair * SPLIT,))] * 6,
                *[dma(((pair + quad) * SPLIT,))] * 2,
            ],
            compiler_params=pltpu.CompilerParams(
                collective_id=0, has_side_effects=True, vmem_limit_bytes=52 * 1024 * 1024
            ),
        )(jnp.stack([col_owner[:, 0], col_cluster, row_cluster, block_ranks]), *arrays)
        return gathered.reshape(field_in.shape).astype(F32)

    held = slots_of(col_owner, owners, most)
    number = jnp.arange(blocks, dtype=jnp.int32)
    halves = [clusters >> (t + 1) for t in range(stages)]
    steps = [
        pltpu.VMEM((PARTS, half, width, part), BF16 if t else F32) for t, half in enumerate(halves)
    ]
    gathered = pl.pallas_call(
        functools.partial(kernel, owners, reps, most),
        out_shape=jax.ShapeDtypeStruct(field_in.shape, BF16),
        in_specs=[smem] + [vmem] * 4,
        out_specs=vmem,
        scratch_shapes=[
            pltpu.VMEM((owners, depth, width), BF16),
            pltpu.VMEM((owners, depth, width), BF16),
            pltpu.VMEM((owners, width, depth), BF16),
            pltpu.VMEM((PARTS, owners, tall, part), BF16),
            pltpu.VMEM((PARTS, owners, tall, part), BF16),
            pltpu.VMEM((2, share, width), BF16),
            pltpu.VMEM((2, share, columns), BF16),
            pltpu.VMEM((PARTS, clusters, width, part), F32),
            *steps,
            *steps,
            dma((owners,)),
            dma((owners,)),
            dma((PARTS, owners)),
            dma((PARTS, owners)),
            dma((4,)),
            dma((4,)),
            *[dma((PARTS, stages))] * 4,
        ],
        compiler_params=pltpu.CompilerParams(
            collective_id=0, has_side_effects=True, vmem_limit_bytes=60 * 1024 * 1024
        ),
    )(table(held, clusters, [number, row_cluster, block_ranks, col_cluster - clusters]), *arrays)
    return gathered.astype(F32)


def solution(mesh):
    in_specs = (
        P("rows", None, None),
        P(("rows", "rep"), None, None),
        P(("rows", "rep"), None, None),
        P(("rows", "rep")),
        P(("rows", "rep")),
        P(("rows", "rep"), None),
        P(("rows", "rep")),
        P("rows", None, "rep", None),
    )
    out_specs = P("rows", None, None)
    return jax.shard_map(shards, mesh=mesh, in_specs=in_specs, out_specs=out_specs, check_vma=False)
```
